32 devices in a mesh: rep: 1 (over z), dp: 32 (over x, y, core).
Axes of the slice: x: 4, y: 4, z: 1, core: 2. Of those that a mesh axis runs over, the one named last changes fastest.
The devices are a block of a 4x4x8 slice.
Arguments:
- x: bfloat16 [32, 2048, 1024], P(('rep', 'dp'))
- dy: bfloat16 [32, 2048, 1024], P(('rep', 'dp'))
- w_gate: bfloat16 [2, 1024, 2560], replicated
- w_up: bfloat16 [2, 1024, 2560], replicated
- w_down: bfloat16 [2, 2560, 1024], replicated
- m_w_gate: float32 [2, 1024, 2560], replicated
- m_w_up: float32 [2, 1024, 2560], replicated
- m_w_down: float32 [2, 2560, 1024], replicated
- v_w_gate: float32 [2, 1024, 2560], replicated
- v_w_up: float32 [2, 1024, 2560], replicated
- v_w_down: float32 [2, 2560, 1024], replicated
Outputs:
- output 1: bfloat16 [2, 1024, 2560], P('rep')
- output 2: bfloat16 [2, 1024, 2560], P('rep')
- output 3: bfloat16 [2, 2560, 1024], P('rep')
- output 4: float32 [2, 1024, 2560], P('rep')
- output 5: float32 [2, 1024, 2560], P('rep')
- output 6: float32 [2, 2560, 1024], P('rep')
- output 7: float32 [2, 1024, 2560], P('rep')
- output 8: float32 [2, 1024, 2560], P('rep')
- output 9: float32 [2, 2560, 1024], P('rep')
All inputs are finite; a program needn't handle non-finite values.
Results may differ from the reference program's by a relative error of at most 0.022.
Values are sent between devices in bfloat16 or wider.
A program may use at most 768 MiB of HBM per device.

```python
import jax
import jax.numpy as jnp
from jax import lax

SEQUENCES = 32
TOKENS = 2048
D = 1024
FF = 2560
LAYERS = 2
NAMES = ("w_gate", "w_up", "w_down")
SHAPES = {"w_gate": (LAYERS, D, FF), "w_up": (LAYERS, D, FF), "w_down": (LAYERS, FF, D)}


def bump(key, n, height):
    away = (jnp.arange(n, dtype=jnp.int32) - jax.random.randint(key, (), 0, n, jnp.int32)) % n
    return jnp.where(away < n // 8, height, 1.0)


def together(key, own, strength):
    shared = jax.random.normal(key, own.shape[1:], jnp.float32)
    return (own + strength * shared) * lax.rsqrt(1 + strength * strength)


def setup_inputs(seed: int = 0, part: int = 0) -> dict:
    kx, kdy, ka, kb, kz, kf, kh, kl, *keys = jax.random.split(jax.random.key(seed), 8 + 3 * len(NAMES))
    kx, kdy, ka, kb = (jax.random.fold_in(k, part) for k in (kx, kdy, ka, kb))
    kw, km, kv = (keys[i::3] for i in range(3))
    shape = (SEQUENCES, TOKENS, D)
    much_x, much_dy = jax.random.uniform(kz, (2,), jnp.float32, 0.0, 1.0)
    loud = 2.0 ** jax.random.uniform(jax.random.fold_in(kz, 1), (), jnp.float32, -1.0, 2.0)
    layers = 2.0 ** jax.random.uniform(kl, (LAYERS, 1, 1), jnp.float32, -1.0, 1.0)
    x = together(ka, jax.random.normal(kx, shape, jnp.float32), much_x) * bump(kf, D, 4.0)
    dy = together(kb, jax.random.normal(kdy, shape, jnp.float32), much_dy)
    drawn = {"x": x.astype(jnp.bfloat16), "dy": (loud * dy * (SEQUENCES * TOKENS) ** -0.5).astype(jnp.bfloat16)}
    for key, name in zip(kw, NAMES, strict=True):
        w = jax.random.normal(key, SHAPES[name], jnp.float32) * SHAPES[name][1] ** -0.5
        drawn[name] = (w * {"w_gate": 1.0, "w_up": bump(kh, FF, 4.0), "w_down": layers}[name]).astype(jnp.bfloat16)
    for key, name in zip(km, NAMES, strict=True):
        drawn[f"m_{name}"] = 0.1 * jax.random.normal(key, SHAPES[name], jnp.float32)
    for key, name in zip(kv, NAMES, strict=True):
        drawn[f"v_{name}"] = jax.random.uniform(key, SHAPES[name], jnp.float32, 0.005, 0.015)
    return drawn


def matmul(a, w):
    return jnp.dot(a, w, preferred_element_type=jnp.float32).astype(jnp.bfloat16)


def normed(h):
    wide = h.astype(jnp.float32)
    scale = lax.rsqrt(jnp.mean(wide**2, -1, keepdims=True) + 1e-6)
    return (wide * scale).astype(jnp.bfloat16)


def layer(h, w):
    a = normed(h)
    gate = jnp.dot(a, w["w_gate"], preferred_element_type=jnp.float32)
    up = jnp.dot(a, w["w_up"], preferred_element_type=jnp.float32)
    return h + matmul((jax.nn.silu(gate) * up).astype(jnp.bfloat16), w["w_down"])


def adamw(w, m, v, g):
    m = 0.9 * m + 0.1 * g
    v = 0.95 * v + 0.05 * g * g
    step = m * lax.rsqrt(v + 1e-8) + 0.1 * w
    return (w - 0.02 * step).astype(jnp.bfloat16), m, v


def clipped(gradients, sum_of_squares, count):
    factor = jnp.minimum(1.0, 0.5 * lax.rsqrt(sum_of_squares / count + 1e-30))
    return [g * factor for g in gradients]


def stack(weights, h):
    return lax.scan(lambda h, w: (layer(h, w), None), h, weights)[0]


def reference(x, dy, w_gate, w_up, w_down, m_w_gate, m_w_up, m_w_down, v_w_gate, v_w_up, v_w_down):
    weights = dict(zip(NAMES, (w_gate, w_up, w_down), strict=True))

    def take(so_far, sequence):
        h, by_y = sequence
        _, back = jax.vjp(lambda w: stack(w, h), weights)
        return jax.tree.map(lambda total, term: total + term.astype(jnp.float32), so_far, back(by_y)[0]), None

    none_yet = {name: jnp.zeros(w.shape, jnp.float32) for name, w in weights.items()}
    by_weights, _ = lax.scan(take, none_yet, (x, dy))
    gradients = [by_weights[name].astype(jnp.bfloat16).astype(jnp.float32) for name in NAMES]
    gradients = clipped(gradients, sum(jnp.sum(g * g) for g in gradients), sum(g.size for g in gradients))
    new = [
        adamw(w.astype(jnp.float32), m, v, g)
        for w, m, v, g in zip((w_gate, w_up, w_down), (m_w_gate, m_w_up, m_w_down), (v_w_gate, v_w_up, v_w_down), gradients, strict=True)
    ]
    return tuple(one[which] for which in range(3) for one in new)
```

```python
import functools
import math

import jax
import jax.numpy as jnp
from jax import lax
from jax.experimental import pallas as pl
from jax.experimental.pallas import tpu as pltpu
from jax.sharding import PartitionSpec as P

F32, BF16 = jnp.float32, jnp.bfloat16
MESH = pl.DeviceIdType.MESH
VLIM = 64 * 1024 * 1024 - 64 * 1024
DMA = pltpu.SemaphoreType.DMA
ONE = dict(pipeline_mode=pl.Buffered(1))


def dot(a, b):
    return jnp.dot(a, b, preferred_element_type=F32)


def dot_t(a, b):
    return lax.dot_general(a, b, (((1,), (1,)), ((), ())), preferred_element_type=F32)


def t_dot(a, b):
    return lax.dot_general(a, b, (((0,), (0,)), ((), ())), preferred_element_type=F32)


def ds(i, size):
    return pl.ds(pl.multiple_of(i * size, size), size)


def norm_rows(h):
    wide = h.astype(F32)
    scale = lax.rsqrt(jnp.mean(wide * wide, -1, keepdims=True) + 1e-6)
    return (wide * scale).astype(BF16)


class Place:
    def __init__(self, side):
        me = lax.axis_index("dp")
        self.core, chip = lax.rem(me, 2), lax.div(me, 2)
        x, y = lax.div(chip, side), lax.rem(chip, side)
        self.side = side
        at = lambda x, y, core: {"dp": (lax.rem(x + side, side) * side + lax.rem(y + side, side)) * 2 + core}
        self.partner = at(x, y, 1 - self.core)
        along_x = [at(x + k, y, self.core) for k in range(side)]
        along_y = [at(x, y + k, self.core) for k in range(side)]
        self.peers = [self.partner, along_x[1], along_x[-1], along_y[1], along_y[-1]]
        self.rings = [along_x, along_y]
        self.positions = [x, y]
        ring = lambda p, r: (p, r[1], r[-1])
        self.first = [ring(x, along_x), ring(y, along_y)]
        self.second = [ring(y, along_y), ring(x, along_x)]

    def on(self, p, k):
        return lax.rem(p + k, self.side)


def remote(src, dst, send, recv, device):
    return pltpu.make_async_remote_copy(src_ref=src, dst_ref=dst, send_sem=send, recv_sem=recv, device_id=device, device_id_type=MESH)


def greet(peers):
    barrier = pltpu.get_barrier_semaphore()
    for peer in peers:
        pl.semaphore_signal(barrier, inc=1, device_id=peer, device_id_type=MESH)
    pl.semaphore_wait(barrier, len(peers))


def fwd_kernel(x_ref, wg_ref, wu_ref, wd_ref, h_ref, a_ref, gate_ref, up_ref, acc_ref, act_ref, *, mc):
    n, steps = pl.program_id(0), pl.num_programs(0)
    tokens = x_ref.shape[0]
    chunks, block = tokens // mc, tokens // 8

    @pl.when(n == 0)
    def _():
        @pl.loop(0, tokens // block)
        def _(i):
            rows = ds(i, block)
            a_ref[rows, :] = norm_rows(x_ref[rows, :])
            acc_ref[rows, :] = jnp.zeros((block, acc_ref.shape[1]), F32)

    def gu(c):
        rows = pl.ds(c * mc, mc)
        a = a_ref[rows, :]
        gate_ref[0, rows, :] = dot(a, wg_ref[0])
        up_ref[0, rows, :] = dot(a, wu_ref[0])

    def epi(c):
        rows = pl.ds(c * mc, mc)
        g, u = gate_ref[0, rows, :], up_ref[0, rows, :]
        act_ref[rows, :] = (g * jax.nn.sigmoid(g) * u).astype(BF16)

    def down(c):
        rows = pl.ds(c * mc, mc)
        acc_ref[rows, :] += dot(act_ref[rows, :], wd_ref[0])

    gu(0)
    for c in range(chunks):
        if c + 1 < chunks:
            gu(c + 1)
        epi(c)
        if c > 0:
            down(c - 1)
    down(chunks - 1)

    @pl.when(n == steps - 1)
    def _():
        @pl.loop(0, tokens // block)
        def _(i):
            rows = ds(i, block)
            y = acc_ref[rows, :].astype(BF16).astype(F32)
            h_ref[rows, :] = (x_ref[rows, :].astype(F32) + y).astype(BF16)


def fwd(x, wg, wu, wd, layer, tn):
    t, d = x.shape
    ff = wg.shape[2]
    whole = pl.BlockSpec((t, d), lambda n: (0, 0), **ONE)
    tile = pl.BlockSpec((1, t, tn), lambda n: (n, 0, 0))
    return pl.pallas_call(
        functools.partial(fwd_kernel, mc=t // 4),
        grid=(ff // tn,),
        in_specs=[
            whole,
            pl.BlockSpec((1, d, tn), lambda n: (layer, 0, n)),
            pl.BlockSpec((1, d, tn), lambda n: (layer, 0, n)),
            pl.BlockSpec((1, tn, d), lambda n: (layer, n, 0)),
        ],
        out_specs=[whole, whole, tile, tile],
        out_shape=[jax.ShapeDtypeStruct((t, d), BF16)] * 2 + [jax.ShapeDtypeStruct((ff // tn, t, tn), F32)] * 2,
        scratch_shapes=[pltpu.VMEM((t, d), F32), pltpu.VMEM((t, tn), BF16)],
        compiler_params=pltpu.CompilerParams(vmem_limit_bytes=VLIM, dimension_semantics=("arbitrary",)),
        cost_estimate=pl.CostEstimate(flops=6 * t * d * ff, bytes_accessed=10 * t * ff, transcendentals=t * ff),
        name="fwd",
    )(x, wg, wu, wd)


def gates(g, u, dact):
    s = jax.nn.sigmoid(g)
    silu = g * s
    act = (silu * u).astype(BF16)
    dup = (dact * silu).astype(BF16)
    dgate = (dact * u * (s + silu * (1.0 - s))).astype(BF16)
    return act, dgate, dup


DEPTH = 3
RING = 4
STAGES = 11


class Exchange:
    def __init__(self, tiles, place, buffers, semaphores, shard_ref, full_ref, sq_ref):
        self.tiles, self.place = tiles, place
        self.own, self.r0, self.ra, self.rb, self.ra2, self.rb2, self.ta, self.tb, self.ta2, self.tb2, self.total = buffers
        self.sems = semaphores
        self.shard, self.full, self.sq = shard_ref, full_ref, sq_ref
        self.rows = self.r0.shape[2] // place.side
        self.sub = self.rows // place.side

    def pair(self, t, name, axis, src, dst):
        send, recv = self.sems[name]
        slot = lax.rem(t, recv.shape[0])
        copies = []
        for o in range(2):
            for k in range(2):
                copies.append(remote(src(o, k), dst(o, k), send.at[o, k], recv.at[slot, o, k], axis[o][1 + k]))
        return copies

    def d2d(self, t):
        send, recv = self.sems["d2d"]
        slot, core = lax.rem(t, DEPTH), self.place.core
        return [remote(self.own.at[slot, 1 - core], self.r0.at[slot], send, recv.at[slot], self.place.partner)]

    def a(self, t):
        half, slot = self.rows // 2, lax.rem(t, DEPTH)
        return self.pair(t, "a", self.place.first, lambda o, k: self.ta.at[o, pl.ds(k * half, half)], lambda o, k: self.ra.at[slot, o, k])

    def b(self, t):
        slot = lax.rem(t, DEPTH)
        return self.pair(t, "b", self.place.first, lambda o, k: self.tb.at[o, k], lambda o, k: self.rb.at[slot, o, k])

    def a2(self, t):
        half, slot = self.sub // 2, lax.rem(t, DEPTH)
        return self.pair(t, "a2", self.place.second, lambda o, k: self.ta2.at[o, pl.ds(k * half, half)], lambda o, k: self.ra2.at[slot, o, k])

    def b2(self, t):
        slot = lax.rem(t, DEPTH)
        return self.pair(t, "b2", self.place.second, lambda o, k: self.tb2.at[o, k], lambda o, k: self.rb2.at[slot, o, k])

    def cell(self, t, o, step):
        p, q = self.place.first[o][0], self.place.second[o][0]
        return self.full.at[t, self.place.core, o, p * self.place.side + self.place.on(q, step)]

    def keep(self, t):
        slot = lax.rem(t, 2)
        return [pltpu.make_async_copy(self.shard.at[t, o], self.cell(t, o, 0), self.sems["keep"].at[slot, o]) for o in range(2)]

    def d(self, t):
        return self.pair(t, "d", self.place.second, lambda o, k: self.shard.at[t, o], lambda o, k: self.cell(t, o, 0))

    def e(self, t):
        half, side = self.sub // 2, self.place.side
        cut = lambda o, k: self.cell(t, o, (side - 1, 1)[k]).at[pl.ds(k * half, half)]
        return self.pair(t, "e", self.place.second, cut, cut)

    def line(self, t, o, step, first, size):
        i = self.place.on(self.place.first[o][0], step)
        return self.full.at[t, self.place.core, o, pl.ds(i * self.place.side + first, size)]

    def f(self, t):
        cut = lambda o, k: self.line(t, o, 0, 0, self.place.side)
        return self.pair(t, "f", self.place.first, cut, cut)

    def g(self, t):
        side = self.place.side
        cut = lambda o, k: self.line(t, o, (side - 1, 1)[k], k * side // 2, side // 2)
        return self.pair(t, "g", self.place.first, cut, cut)

    def h(self, t):
        send, recv = self.sems["h"]
        half = self.full.at[t, self.place.core]
        return [remote(half, half, send, recv.at[lax.rem(t, RING)], self.place.partner)]

    def chip(self, t, o, first, count):
        at, slot = pl.ds(pl.multiple_of(first, count), count), lax.rem(t, DEPTH)
        return self.own[slot, self.place.core, o, at, :].astype(F32) + self.r0[slot, o, at, :].astype(F32)

    def sum_a(self, t):
        for o in range(2):
            chunk = self.place.on(self.place.first[o][0], 2)
            for i in range(0, self.rows, self.sub):
                self.ta[o, i:i + self.sub, :] = self.chip(t, o, chunk * self.rows + i, self.sub).astype(BF16)

    def sum_b(self, t):
        slot, half, side = lax.rem(t, DEPTH), self.rows // 2, self.place.side
        for o in range(2):
            for k in range(2):
                chunk = self.place.on(self.place.first[o][0], (1, side - 1)[k])
                for i in range(0, self.rows, self.sub):
                    x = self.chip(t, o, chunk * self.rows + i, self.sub)
                    if i // half == k:
                        x = x + self.ra[slot, o, k, i - k * half:i - k * half + self.sub, :].astype(F32)
                    self.tb[o, k, i:i + self.sub, :] = x.astype(BF16)

    def sum_a2(self, t):
        slot, keep = lax.rem(t, DEPTH), lax.rem(t, 2)
        for o in range(2):
            chunk = self.place.first[o][0]
            for i in range(0, self.rows, self.sub):
                x = self.chip(t, o, chunk * self.rows + i, self.sub)
                for k in range(2):
                    x = x + self.rb[slot, o, k, i:i + self.sub, :].astype(F32)
                self.total[keep, o, i:i + self.sub, :] = x
            self.ta2[o] = self.total[keep, o, ds(self.place.on(self.place.second[o][0], 2), self.sub), :].astype(BF16)

    def sum_b2(self, t):
        slot, keep, half, side = lax.rem(t, DEPTH), lax.rem(t, 2), self.sub // 2, self.place.side
        for o in range(2):
            for k in range(2):
                chunk = self.place.on(self.place.second[o][0], (1, side - 1)[k])
                for i in range(2):
                    x = self.total[keep, o, pl.ds(pl.multiple_of(chunk * self.sub + i * half, half), half), :]
                    if i == k:
                        x = x + self.ra2[slot, o, k].astype(F32)
                    self.tb2[o, k, i * half:(i + 1) * half, :] = x.astype(BF16)

    def finish(self, t):
        slot, keep = lax.rem(t, DEPTH), lax.rem(t, 2)
        for o in range(2):
            x = self.total[keep, o, ds(self.place.second[o][0], self.sub), :]
            for k in range(2):
                x = x + self.rb2[slot, o, k].astype(F32)
            g = x.astype(BF16)
            self.shard[t, o] = g
            g = g.astype(F32)
            self.sq[...] += g * g
        for copy in self.keep(t):
            copy.start()

    def kept(self, t):
        for copy in self.keep(t):
            copy.wait()

    def left(self, t):
        @pl.when(t == self.tiles - 1)
        def _():
            for copy in self.h(t):
                copy.wait_send()

    def stage(self, n, k, start, before=None, work=None):
        t = n - k
        if start is not None:
            @pl.when((t >= 1) & (t <= self.tiles))
            def _():
                for copy in start(t - 1):
                    copy.wait_send()

        @pl.when((t >= 0) & (t < self.tiles))
        def _():
            if before is not None:
                for copy in before(t):
                    copy.wait_recv()
            if work is not None:
                work(t)
            if start is not None:
                for copy in start(t):
                    copy.start()

    def inside(self, n):
        self.stage(n, 1, self.a, self.d2d, self.sum_a)
        self.stage(n, 2, self.a2, self.b, self.sum_a2)
        self.stage(n, 3, self.d, self.b2, self.finish)
        self.stage(n, 4, self.f, self.e, self.kept)
        self.stage(n, 5, self.h, self.g)

    def after(self, n):
        self.stage(n, 0, self.d2d)
        self.stage(n, 1, self.b, self.a, self.sum_b)
        self.stage(n, 2, self.b2, self.a2, self.sum_b2)
        self.stage(n, 3, self.e, self.d)
        self.stage(n, 4, self.g, self.f)
        self.stage(n, 5, None, self.h, self.left)


class Total:
    def __init__(self, place, sums, send, recv):
        self.place, self.sums, self.send, self.recv = place, sums, send, recv
        self.members = [[None, place.partner], *place.rings]
        self.me = [place.core, *place.positions]

    def copies(self, k):
        here = self.sums.at[k, self.me[k]]
        return [remote(here, here, self.send.at[k, i], self.recv.at[k, i], peer) for i, peer in enumerate(self.members[k]) if i]

    def start(self, k, value):
        self.sums[k, self.me[k]] = value
        for copy in self.copies(k):
            copy.start()

    def end(self, k):
        for copy in self.copies(k):
            copy.wait()
        value = self.sums[k, 0]
        for i in range(1, len(self.members[k])):
            value = value + self.sums[k, i]
        return value


def grads_kernel(h_ref, dy_ref, wg_ref, wu_ref, wd_ref, a0_hbm, gate_hbm, up_hbm, full_ref, factor_ref,
                 a_ref, a0_ref, da_ref, g_ref, u_ref, dact_ref, act_ref, dgu_ref,
                 own, r0, ra, rb, ra2, rb2, ta, tb, ta2, tb2, total, shard_ref, sq_ref, sums,
                 a0_sem, gu_sem, vs, vr, keep_sem, s0, q0, sh, qh, *pairs, mc, side, tiles, count):
    n = pl.program_id(0)
    tokens, d = h_ref.shape
    tn = wg_ref.shape[2]
    chunks, block = tokens // mc, tokens // 8
    place = Place(side)
    piece = d // (2 * side * side)
    sems = {name: pairs[2 * i:2 * i + 2] for i, name in enumerate(("a", "b", "a2", "b2", "d", "e", "f", "g"))}
    sems.update(d2d=(s0, q0), h=(sh, qh), keep=keep_sem)
    exchange = Exchange(
        2 * tiles, place, (own, r0, ra, rb, ra2, rb2, ta, tb, ta2, tb2, total), sems, shard_ref, full_ref, sq_ref
    )
    squares = Total(place, sums, vs, vr)

    def load_a0():
        return pltpu.make_async_copy(a0_hbm, a0_ref, a0_sem)

    def load_gu(t):
        slot = lax.rem(t + 1, 2)
        return (
            pltpu.make_async_copy(gate_hbm.at[t], g_ref.at[slot], gu_sem.at[slot, 0]),
            pltpu.make_async_copy(up_hbm.at[t], u_ref.at[slot], gu_sem.at[slot, 1]),
        )

    @pl.when(n == 0)
    def _():
        load_a0().start()
        greet([place.partner, *place.rings[0][1:], *place.rings[1][1:]])
        sq_ref[...] = jnp.zeros_like(sq_ref)

        @pl.loop(0, tokens // block)
        def _(i):
            rows = ds(i, block)
            a_ref[rows, :] = norm_rows(h_ref[rows, :])
            da_ref[rows, :] = jnp.zeros((block, d), F32)

    @pl.when((n >= tiles - 1) & (n < 2 * tiles - 1))
    def _():
        for copy in load_gu(n + 1 - tiles):
            copy.start()

    def weights_down(act, right):
        slot = lax.rem(n, DEPTH)
        down = t_dot(act[...], right[...]).astype(BF16)
        lanes = d // (2 * side)
        for o in range(2):
            for c in range(2):
                for i in range(side):
                    for j in range(side):
                        k = (i * side + j) * piece
                        own[slot, c, o, k:k + piece, tn:] = down[
                            (o * side + i) * piece:(o * side + i + 1) * piece, (c * side + j) * lanes:(c * side + j + 1) * lanes
                        ]

    def weights_in(left, dgu):
        slot, half = lax.rem(n, DEPTH), d // 2
        for c in range(2):
            at = left[:, c * half:(c + 1) * half]
            own[slot, c, 0, :, :tn] = t_dot(at, dgu[:, :tn]).astype(BF16)
            own[slot, c, 1, :, :tn] = t_dot(at, dgu[:, tn:]).astype(BF16)

    def epi(c, g, u):
        rows = pl.ds(c * mc, mc)
        dact = dact_ref[rows, :].astype(BF16).astype(F32)
        act, dgate, dup = gates(g[rows, :], u[rows, :], dact)
        act_ref[rows, :] = act
        dgu_ref[rows, :tn] = dgate
        dgu_ref[rows, tn:] = dup

    last, first = n < tiles, (n >= tiles) & (n < 2 * tiles)

    @pl.when(last)
    def _():
        def gud(c):
            rows = pl.ds(c * mc, mc)
            a = a_ref[rows, :]
            g_ref[0, rows, :] = dot(a, wg_ref[0])
            u_ref[0, rows, :] = dot(a, wu_ref[0])
            dact_ref[rows, :] = dot_t(dy_ref[rows, :], wd_ref[0])

        def back(c):
            rows = pl.ds(c * mc, mc)
            da_ref[rows, :] += dot_t(dgu_ref[rows, :tn], wg_ref[0]) + dot_t(dgu_ref[rows, tn:], wu_ref[0])

        gud(0)
        for c in range(1, chunks):
            gud(c)
            epi(c - 1, g_ref.at[0], u_ref.at[0])
        for c in range(chunks - 1):
            back(c)
            if c == 0:
                epi(chunks - 1, g_ref.at[0], u_ref.at[0])
        back(chunks - 1)

    @pl.when(first)
    def _():
        t = n - tiles
        slot = lax.rem(t + 1, 2)
        for copy in load_gu(t):
            copy.wait()

        def da(c):
            rows = pl.ds(c * mc, mc)
            dact_ref[rows, :] = dot_t(a_ref[rows, :], wd_ref[0])

        da(0)
        for c in range(1, chunks):
            da(c)
            epi(c - 1, g_ref.at[slot], u_ref.at[slot])
        epi(chunks - 1, g_ref.at[slot], u_ref.at[slot])
        weights_down(act_ref, a_ref)

    exchange.inside(n)

    @pl.when(n == 2 * tiles + 2)
    def _():
        squares.start(0, jnp.full(factor_ref.shape, jnp.sum(sq_ref[...]), F32))

    @pl.when(n == 2 * tiles + 3)
    def _():
        squares.start(2, squares.end(1))

    @pl.when(last)
    def _():
        weights_down(act_ref, dy_ref)
        weights_in(a_ref, dgu_ref)

    @pl.when(first)
    def _():
        weights_in(a0_ref, dgu_ref)

    exchange.after(n)

    @pl.when(n == tiles - 1)
    def _():
        @pl.loop(0, tokens // block)
        def _(i):
            rows = ds(i, block)
            da = da_ref[rows, :].astype(BF16).astype(F32)
            h = h_ref[rows, :].astype(F32)
            ms = jnp.mean(h * h, -1, keepdims=True) + 1e-6
            r = lax.rsqrt(ms)
            along = jnp.mean(da * h, -1, keepdims=True)
            dn = (r * (da - h * (along / ms))).astype(BF16).astype(F32)
            a_ref[rows, :] = (dy_ref[rows, :].astype(F32) + dn).astype(BF16)

        load_a0().wait()

    @pl.when(n == 2 * tiles + 2)
    def _():
        squares.start(1, squares.end(0))

    @pl.when(n == 2 * tiles + 3)
    def _():
        factor_ref[...] = jnp.minimum(1.0, 0.5 * lax.rsqrt(squares.end(2) / count + 1e-30))


def grads(h, dy, wg, wu, wd, a0, gate, up, tn, side, count):
    t, d = h.shape
    ff = wg.shape[2]
    tiles = ff // tn
    piece, wide = d // (2 * side * side), tn + d // (2 * side)
    chunk = side * piece
    rows = side * chunk
    whole = pl.BlockSpec((t, d), lambda n: (0, 0), **ONE)
    hbm = pl.BlockSpec(memory_space=pl.ANY)
    mid = lambda n: jnp.minimum(n, tiles - 1)
    full = (2 * tiles, 2, 2, side * side, piece, wide)
    return pl.pallas_call(
        functools.partial(grads_kernel, mc=t // 4, side=side, tiles=tiles, count=count),
        grid=(2 * tiles + 5,),
        in_specs=[
            whole,
            whole,
            pl.BlockSpec((1, d, tn), lambda n: (1, 0, mid(n))),
            pl.BlockSpec((1, d, tn), lambda n: (1, 0, mid(n))),
            pl.BlockSpec((1, tn, d), lambda n: (jnp.where(n < tiles, 1, 0), jnp.where(n < tiles, n, jnp.minimum(n - tiles, tiles - 1)), 0)),
            hbm,
            hbm,
            hbm,
        ],
        out_specs=[hbm, pl.BlockSpec((8, 128), lambda n: (0, 0), **ONE)],
        out_shape=[jax.ShapeDtypeStruct(full, BF16), jax.ShapeDtypeStruct((8, 128), F32)],
        scratch_shapes=[
            pltpu.VMEM((t, d), BF16), pltpu.VMEM((t, d), BF16), pltpu.VMEM((t, d), F32),
            pltpu.VMEM((2, t, tn), F32), pltpu.VMEM((2, t, tn), F32), pltpu.VMEM((t, tn), F32),
            pltpu.VMEM((t, tn), BF16), pltpu.VMEM((t, 2 * tn), BF16),
            pltpu.VMEM((DEPTH, 2, 2, rows, wide), BF16),
            pltpu.VMEM((DEPTH, 2, rows, wide), BF16),
            pltpu.VMEM((DEPTH, 2, 2, chunk // 2, wide), BF16),
            pltpu.VMEM((DEPTH, 2, 2, chunk, wide), BF16),
            pltpu.VMEM((DEPTH, 2, 2, piece // 2, wide), BF16),
            pltpu.VMEM((DEPTH, 2, 2, piece, wide), BF16),
            pltpu.VMEM((2, chunk, wide), BF16),
            pltpu.VMEM((2, 2, chunk, wide), BF16),
            pltpu.VMEM((2, piece, wide), BF16),
            pltpu.VMEM((2, 2, piece, wide), BF16),
            pltpu.VMEM((2, 2, chunk, wide), F32),
            pltpu.VMEM((2 * tiles, 2, piece, wide), BF16),
            pltpu.VMEM((piece, wide), F32),
            pltpu.VMEM((3, side, 8, 128), F32),
            DMA, DMA((2, 2)), DMA((3, side)), DMA((3, side)), DMA((2, 2)),
            DMA, DMA((DEPTH,)), DMA, DMA((RING,)),
            *[sem for name in range(4) for sem in (DMA((2, 2)), DMA((DEPTH, 2, 2)))],
            *[sem for name in range(4) for sem in (DMA((2, 2)), DMA((RING, 2, 2)))],
        ],
        compiler_params=pltpu.CompilerParams(
            vmem_limit_bytes=VLIM, dimension_semantics=("arbitrary",), collective_id=0, has_side_effects=True
        ),
        cost_estimate=pl.CostEstimate(flops=24 * t * d * ff, bytes_accessed=20 * d * ff, transcendentals=2 * t * ff),
        name="grads",
    )(h, dy, wg, wu, wd, a0, gate, up)


def adam_kernel(factor_ref, full_ref, *refs, side):
    weights, moments, squares, new_w, new_m, new_v = (refs[i:i + 3] for i in range(0, 18, 3))
    part = pl.program_id(1)
    piece, wide = full_ref.shape[4:]
    tn = new_w[0].shape[2]
    lanes = wide - tn
    f = factor_ref[0, 0]

    def step(k, at, g):
        g = g.astype(F32) * f
        m = 0.9 * moments[k][at] + 0.1 * g
        v = 0.95 * squares[k][at] + 0.05 * (g * g)
        w = weights[k][at].astype(F32)
        new_w[k][at] = (w - 0.02 * (m * lax.rsqrt(v + 1e-8) + 0.1 * w)).astype(BF16)
        new_m[k][at] = m
        new_v[k][at] = v

    @pl.loop(0, side)
    def _(i):
        for j in range(side):
            rows = ds(i * side + j, piece)
            for o in range(2):
                step(o, (0, rows, slice(None)), full_ref[0, part, o, i * side + j, :, :tn])
        rows = ds(i, piece)
        for c in range(2):
            for j in range(side):
                at = (0, rows, slice((c * side + j) * lanes, (c * side + j + 1) * lanes))
                step(2, at, full_ref[0, c, part, i * side + j, :, tn:])


def adam(factor, full, ws, ms, vs, tn, side):
    _, d, ff = ws[0].shape
    tiles = ff // tn
    layer = lambda t: 1 - t // tiles
    up = pl.BlockSpec((1, d // 2, tn), lambda t, c: (layer(t), c, t % tiles))
    down = pl.BlockSpec((1, tn // 2, d), lambda t, c: (layer(t), (t % tiles) * 2 + c, 0))
    blocks = [up, up, down]
    size = sum(w.size for w in ws)
    out = pl.pallas_call(
        functools.partial(adam_kernel, side=side),
        grid=(2 * tiles, 2),
        in_specs=[
            pl.BlockSpec(factor.shape, lambda t, c: (0, 0), **ONE),
            pl.BlockSpec((1, *full.shape[1:]), lambda t, c: (t, 0, 0, 0, 0, 0)),
            *blocks * 3,
        ],
        out_specs=blocks * 3,
        out_shape=[jax.ShapeDtypeStruct(a.shape, a.dtype) for a in (*ws, *ms, *vs)],
        compiler_params=pltpu.CompilerParams(vmem_limit_bytes=VLIM, dimension_semantics=("arbitrary", "arbitrary")),
        cost_estimate=pl.CostEstimate(flops=20 * size, bytes_accessed=22 * size, transcendentals=size),
        name="adam",
    )(factor, full, *ws, *ms, *vs)
    return tuple(out)


def solution(mesh):
    side = math.isqrt(mesh.shape["dp"] // 2)

    def step(x, dy, *arrays):
        ws, ms, vs = (arrays[i:i + 3] for i in (0, 3, 6))
        wg, wu, wd = ws
        x, dy = x[0], dy[0]
        tn = x.shape[1] // side
        h, a0, gate, up = fwd(x, wg, wu, wd, 0, tn)
        full, factor = grads(h, dy, wg, wu, wd, a0, gate, up, tn, side, sum(w.size for w in ws))
        return adam(factor, full, ws, ms, vs, tn, side)

    return jax.shard_map(
        step,
        mesh=mesh,
        in_specs=(P(("rep", "dp"), None, None),) * 2 + (P(None, None, None),) * 9,
        out_specs=(P("rep", None, None),) * 9,
        check_vma=False,
    )
```

```python
import functools
import math

import jax
import jax.numpy as jnp
from jax import lax
from jax.experimental import pallas as pl
from jax.experimental.pallas import tpu as pltpu
from jax.sharding import PartitionSpec as P

F32, BF16 = jnp.float32, jnp.bfloat16
MESH = pl.DeviceIdType.MESH
VLIM = 64 * 1024 * 1024 - 64 * 1024
DMA = pltpu.SemaphoreType.DMA
ONE = dict(pipeline_mode=pl.Buffered(1))


def dot(a, b):
    return jnp.dot(a, b, preferred_element_type=F32)


def dot_t(a, b):
    return lax.dot_general(a, b, (((1,), (1,)), ((), ())), preferred_element_type=F32)


def t_dot(a, b):
    return lax.dot_general(a, b, (((0,), (0,)), ((), ())), preferred_element_type=F32)


def ds(i, size):
    return pl.ds(pl.multiple_of(i * size, size), size)


def norm_rows(h):
    wide = h.astype(F32)
    scale = lax.rsqrt(jnp.mean(wide * wide, -1, keepdims=True) + 1e-6)
    return (wide * scale).astype(BF16)


class Place:
    def __init__(self, side):
        me = lax.axis_index("dp")
        self.core, chip = lax.rem(me, 2), lax.div(me, 2)
        x, y = lax.div(chip, side), lax.rem(chip, side)
        self.side = side
        at = lambda x, y, core: {"dp": (lax.rem(x + side, side) * side + lax.rem(y + side, side)) * 2 + core}
        self.partner = at(x, y, 1 - self.core)
        along_x = [at(x + k, y, self.core) for k in range(side)]
        along_y = [at(x, y + k, self.core) for k in range(side)]
        self.peers = [self.partner, along_x[1], along_x[-1], along_y[1], along_y[-1]]
        self.rings = [along_x, along_y]
        self.positions = [x * 2 + self.core, y]
        self.members = [[at(x + r // 2, y, lax.rem(self.core + r % 2, 2)) for r in range(2 * side)], along_y]
        ring = lambda p, r: (p, r[1], r[-1])
        self.first = [ring(x, along_x), ring(y, along_y)]
        self.second = [ring(y, along_y), ring(x, along_x)]

    def on(self, p, k):
        return lax.rem(p + k, self.side)


def remote(src, dst, send, recv, device):
    return pltpu.make_async_remote_copy(src_ref=src, dst_ref=dst, send_sem=send, recv_sem=recv, device_id=device, device_id_type=MESH)


def greet(peers):
    barrier = pltpu.get_barrier_semaphore()
    for peer in peers:
        pl.semaphore_signal(barrier, inc=1, device_id=peer, device_id_type=MESH)
    pl.semaphore_wait(barrier, len(peers))


OWN = 4
MATE = 4
DEPTH = 2
GROUP = 2
FINISH = 5


class Exchange:
    def __init__(self, tiles, gathered, place, buffers, semaphores, shard_ref, full_ref, rest_ref, sq_ref):
        self.tiles, self.gathered, self.place = tiles, gathered, place
        self.early = tiles // 2
        self.own, self.mate, self.out, self.inn, self.total = buffers
        self.sems = semaphores
        self.shard, self.full, self.rest, self.sq = shard_ref, full_ref, rest_ref, sq_ref
        self.rows = self.mate.shape[2] // place.side
        self.sub = self.rows // place.side
        half, small = self.rows // 2, self.sub // 2
        self.a, self.a2, self.b2, self.b = 0, half, half + small, half + small + self.sub

    def tile(self, tick):
        two = tick < 2 * self.early
        there = (tick >= 0) & (tick < self.tiles + self.early) & ((lax.rem(tick + 4 * self.tiles, 2) == 1) | jnp.logical_not(two))
        return jnp.where(two, lax.div(tick, 2), tick - self.early), there

    def neighbours(self):
        return [(axis, k, self.place.first[axis][1 + k]) for axis in range(2) for k in range(2)]

    def ring(self, tick, first, stop):
        slot = lax.rem(tick, DEPTH)
        send, recv = self.sems["ring"]
        rows = pl.ds(first, stop - first)
        return [
            remote(self.out.at[i, k, rows], self.inn.at[slot, i, k, rows], send, recv.at[slot], peer) for i, k, peer in self.neighbours()
        ]

    def ring_all(self, tick, first, stop, which):
        slot = lax.rem(tick, DEPTH)
        ref = self.inn.at[slot, :, :, pl.ds(first, stop - first)]
        send, recv = self.sems["ring"]
        return pltpu.make_async_copy(ref, ref, send if which == 0 else recv.at[slot])

    def in_parts(self, tick, what):
        end, middle, last = self.b + self.rows, 2 * self.early, self.tiles + self.early
        odd = lax.rem(tick + 2, 2) == 1
        for when, first, stop in (
            ((tick >= 0) & (tick < middle) & jnp.logical_not(odd), self.a, self.b2),
            ((tick >= 0) & (tick < middle) & odd, self.b2, end),
            ((tick >= middle) & (tick <= last), self.a, end),
            (tick == last + 1, self.a2, end),
            (tick == last + 2, self.a2, self.b),
            (tick == last + 3, self.b2, self.b),
        ):
            pl.when(when)(functools.partial(what, first, stop))

    def d2d(self, t):
        send, recv = self.sems["d2d"]
        two, mate = lax.rem(t, 2), lax.rem(t, MATE)
        return remote(self.own.at[OWN + two], self.mate.at[mate], send.at[two], recv.at[mate], self.place.partner)

    def chip(self, t, o, first, count):
        at = pl.ds(pl.multiple_of(first, count), count)
        return self.own[lax.rem(t, OWN), o, at, :].astype(F32) + self.mate[lax.rem(t, MATE), o, at, :].astype(F32)

    def sum_a(self, t, slot):
        half = self.rows // 2
        for o in range(2):
            chunk = self.place.on(self.place.first[o][0], 2)
            for i in range(0, self.rows, self.sub):
                at = self.a + i % half
                self.out[o, i // half, at:at + self.sub, :] = self.chip(t, o, chunk * self.rows + i, self.sub).astype(BF16)

    def sum_b(self, t, slot, k):
        half, side = self.rows // 2, self.place.side
        for o in range(2):
            chunk = self.place.on(self.place.first[o][0], (1, side - 1)[k])
            for i in range(0, self.rows, self.sub):
                x = self.chip(t, o, chunk * self.rows + i, self.sub)
                if i // half == k:
                    at = self.a + i % half
                    x = x + self.inn[slot, o, k, at:at + self.sub, :].astype(F32)
                at = self.b + i
                self.out[o, k, at:at + self.sub, :] = x.astype(BF16)

    def sum_a2(self, t, slot, o):
        keep, half = lax.rem(t, DEPTH), self.sub // 2
        chunk = self.place.first[o][0]
        for i in range(0, self.rows, self.sub):
            x = self.chip(t, o, chunk * self.rows + i, self.sub)
            at = self.b + i
            for k in range(2):
                x = x + self.inn[slot, o, k, at:at + self.sub, :].astype(F32)
            self.total[keep, o, i:i + self.sub, :] = x
        far = self.place.on(self.place.second[o][0], 2)
        for k in range(2):
            x = self.total[keep, o, pl.ds(pl.multiple_of(far * self.sub + k * half, half), half), :]
            self.out[1 - o, k, self.a2:self.a2 + half, :] = x.astype(BF16)

    def sum_b2(self, t, slot):
        keep, half, side = lax.rem(t, DEPTH), self.sub // 2, self.place.side
        for o in range(2):
            for k in range(2):
                chunk = self.place.on(self.place.second[o][0], (1, side - 1)[k])
                for i in range(2):
                    x = self.total[keep, o, pl.ds(pl.multiple_of(chunk * self.sub + i * half, half), half), :]
                    if i == k:
                        x = x + self.inn[slot, 1 - o, k, self.a2:self.a2 + half, :].astype(F32)
                    at = self.b2 + i * half
                    self.out[1 - o, k, at:at + half, :] = x.astype(BF16)

    def finish(self, t, slot):
        keep = lax.rem(t, DEPTH)
        for o in range(2):
            x = self.total[keep, o, ds(self.place.second[o][0], self.sub), :]
            for k in range(2):
                x = x + self.inn[slot, 1 - o, k, self.b2:self.b2 + self.sub, :].astype(F32)
            g = x.astype(BF16)
            self.shard[t, o] = g
            g = g.astype(F32)
            self.sq[...] += g * g

        @pl.when(t >= self.gathered)
        def _():
            self.rest[t - self.gathered] = self.shard[t]

    def tiles_of(self, q):
        return pl.ds(q * GROUP, GROUP)

    def cell(self, q, o, step):
        p, at = self.place.first[o][0], self.place.second[o][0]
        return self.full.at[self.tiles_of(q), self.place.core, o, p * self.place.side + self.place.on(at, step)]

    def line(self, q, o, step, first, size):
        i = self.place.on(self.place.first[o][0], step)
        return self.full.at[self.tiles_of(q), self.place.core, o, pl.ds(i * self.place.side + first, size)]

    def keep(self, q):
        return [
            pltpu.make_async_copy(self.shard.at[self.tiles_of(q), o], self.cell(q, o, 0), self.sems["keep"].at[lax.rem(q, DEPTH), o])
            for o in range(2)
        ]

    def gather(self, name, q):
        send, recv = self.sems[name]
        recv = recv.at[lax.rem(q, DEPTH)]
        side, half = self.place.side, self.sub // 2
        if name == "h":
            both = self.full.at[self.tiles_of(q), self.place.core]
            return [remote(both, both, send, recv, self.place.partner)]
        copies = []
        for o in range(2):
            for k in range(2):
                back = (side - 1, 1)[k]
                if name == "d":
                    src, dst = self.shard.at[self.tiles_of(q), o], self.cell(q, o, 0)
                elif name == "e":
                    p, at = self.place.first[o][0], self.place.second[o][0]
                    src = dst = self.full.at[
                        self.tiles_of(q), self.place.core, o, p * side + self.place.on(at, back), pl.ds(k * half, half)
                    ]
                elif name == "f":
                    src = dst = self.line(q, o, 0, 0, side)
                else:
                    src = dst = self.line(q, o, back, k * side // 2, side // 2)
                axis = self.place.second if name in "de" else self.place.first
                copies.append(remote(src, dst, send, recv, axis[o][1 + k]))
        return copies

    def gather_all(self, name, q, which):
        send, recv = self.sems[name]
        side = self.place.side
        if name == "d":
            ref = self.shard.at[pl.ds(0, 2 * GROUP)]
        elif name == "e":
            ref = self.shard.at[pl.ds(0, GROUP)]
        elif name == "f":
            ref = self.full.at[pl.ds(0, GROUP), 0, 0]
        elif name == "g":
            ref = self.full.at[pl.ds(0, GROUP), 0, 0, pl.ds(0, side * side // 2)]
        else:
            ref = self.full.at[pl.ds(0, GROUP), 0]
        return pltpu.make_async_copy(ref, ref, send if which == 0 else recv.at[lax.rem(q, DEPTH)])

    def gather_step(self, tick, i, before, after):
        t, there = self.tile(tick - FINISH - 1 - i)
        q = lax.div(t, GROUP)

        @pl.when(there & (t < self.gathered) & (lax.rem(t, GROUP) == GROUP - 1))
        def _():
            if before:
                self.gather_all(before, q, 1).wait()
                self.gather_all(before, q, 0).wait()
            if after == "f":
                for copy in self.keep(q):
                    copy.wait()
            if after:
                for copy in self.gather(after, q):
                    copy.start()
            if after == "d":
                for copy in self.keep(q):
                    copy.start()

    def tick(self, tick):
        def ring_wait(first, stop):
            self.ring_all(tick - 1, first, stop, 1).wait()
            self.ring_all(tick - 1, first, stop, 0).wait()

        def ring_start(first, stop):
            for copy in self.ring(tick, first, stop):
                copy.start()

        slot = lax.rem(tick + 1, DEPTH)
        self.in_parts(tick - 1, ring_wait)

        t5, there = self.tile(tick - FINISH)
        pl.when(there)(lambda: self.finish(t5, slot))

        t, there = self.tile(tick - 2)

        @pl.when(there)
        def _():
            self.sum_b(t, slot, 0)
            self.sum_b(t, slot, 1)

        t1, there = self.tile(tick - 1)

        @pl.when(there)
        def _():
            self.d2d(t1).wait_recv()
            self.d2d(t1).wait_send()
            self.sum_a(t1, slot)

        t3, there = self.tile(tick - 3)

        @pl.when(there)
        def _():
            self.sum_a2(t3, slot, 0)
            self.sum_a2(t3, slot, 1)

        t4, there = self.tile(tick - 4)

        @pl.when(there)
        def _():
            self.sum_b2(t4, slot)

        t0, there = self.tile(tick)

        @pl.when(there)
        def _():
            self.d2d(t0).start()

        self.in_parts(tick, ring_start)

        stages = ("d", "e", "f", "g", "h", "")
        for i in reversed(range(6)):
            self.gather_step(tick, i, stages[i - 1] if i else "", stages[i])


class Total:
    def __init__(self, place, sums, send, recv):
        self.place, self.sums, self.send, self.recv = place, sums, send, recv

    def over(self, k, value):
        members, me = self.place.members[k], self.place.positions[k]
        self.sums[k, me] = value
        here = self.sums.at[k, me]
        copies = [remote(here, here, self.send.at[k, i], self.recv.at[k, i], peer) for i, peer in enumerate(members) if i]
        for copy in copies:
            copy.start()
        for copy in copies:
            copy.wait()
        value = self.sums[k, 0]
        for i in range(1, len(members)):
            value = value + self.sums[k, i]
        return value


def gates(g, u, dact):
    s = jax.nn.sigmoid(g)
    silu = g * s
    act = (silu * u).astype(BF16)
    dup = (dact * silu).astype(BF16)
    dgate = (dact * u * (s + silu * (1.0 - s))).astype(BF16)
    return act, dgate, dup


def layers_kernel(x_hbm, dy_hbm, wg_ref, wu_ref, wd_ref, full_ref, rest_ref, factor_ref, gate_hbm, up_hbm,
                  dy_ref, h_ref, a_ref, a0_ref, acc_ref, g_ref, u_ref, dact_ref, act_ref, dgu_ref,
                  own, mate, out, inn, total, shard_ref, sq_ref, sums,
                  x_sem, dy_sem, gu_sem, vs, vr, keep_sem, *pairs, mc, side, tiles, gathered, count):
    step = pl.program_id(0)
    n = step - tiles
    tokens, d = h_ref.shape
    tn = wg_ref.shape[2]
    chunks, blocks = tokens // mc, x_sem.shape[0]
    block = tokens // blocks
    place = Place(side)
    piece = d // (2 * side * side)
    sems = {name: pairs[2 * i:2 * i + 2] for i, name in enumerate(("d2d", "ring", "d", "e", "f", "g", "h"))}
    sems["keep"] = keep_sem
    exchange = Exchange(2 * tiles, gathered, place, (own, mate, out, inn, total), sems, shard_ref, full_ref, rest_ref, sq_ref)

    def load_x(i):
        rows = ds(i, block)
        return pltpu.make_async_copy(x_hbm.at[rows], h_ref.at[rows], x_sem.at[i])

    def load_dy():
        return pltpu.make_async_copy(dy_hbm, dy_ref, dy_sem)

    def put_gu(t):
        slot = lax.rem(t, 2)
        return (
            pltpu.make_async_copy(g_ref.at[slot], gate_hbm.at[t], gu_sem.at[slot, 0]),
            pltpu.make_async_copy(u_ref.at[slot], up_hbm.at[t], gu_sem.at[slot, 1]),
        )

    def get_gu(t):
        slot = lax.rem(t + 1, 2)
        return (
            pltpu.make_async_copy(gate_hbm.at[t], g_ref.at[slot], gu_sem.at[slot, 0]),
            pltpu.make_async_copy(up_hbm.at[t], u_ref.at[slot], gu_sem.at[slot, 1]),
        )

    @pl.when(step == 0)
    def _():
        for i in range(blocks):
            load_x(i).start()
        load_dy().start()
        greet([*place.members[0][1:], *place.members[1][1:]])
        sq_ref[...] = jnp.zeros_like(sq_ref)

        @pl.loop(0, blocks)
        def _(i):
            rows = ds(i, block)
            load_x(i).wait()
            a0_ref[rows, :] = norm_rows(h_ref[rows, :])
            acc_ref[rows, :] = jnp.zeros((block, d), F32)

    @pl.when((step >= 2) & (step <= tiles))
    def _():
        for copy in put_gu(step - 2):
            copy.wait()

    @pl.when(n == 0)
    def _():
        for copy in put_gu(tiles - 1):
            copy.wait()
        load_dy().wait()

    @pl.when((n >= tiles - 1) & (n < 2 * tiles - 1))
    def _():
        for copy in get_gu(n + 1 - tiles):
            copy.start()

    def gu(c, a, slot):
        rows = pl.ds(c * mc, mc)
        a = a[rows, :]
        g_ref[slot, rows, :] = dot(a, wg_ref[0])
        u_ref[slot, rows, :] = dot(a, wu_ref[0])

    def da(c, right):
        dact_ref[c % 2] = dot_t(right[pl.ds(c * mc, mc), :], wd_ref[0])

    def epi(c, slot):
        rows = pl.ds(c * mc, mc)
        dact = dact_ref[c % 2].astype(BF16).astype(F32)
        act, dgate, dup = gates(g_ref[slot, rows, :], u_ref[slot, rows, :], dact)
        act_ref[rows, :] = act
        dgu_ref[rows, :tn] = dgate
        dgu_ref[rows, tn:] = dup

    term = [jnp.where(place.core == c, lax.rem(n + 2 * OWN, OWN), OWN + lax.rem(n + 2 * OWN, 2)) for c in range(2)]

    def weights_down(right):
        lanes = d // (2 * side)
        down = t_dot(act_ref[...], right[...]).astype(BF16)
        for o in range(2):
            for c in range(2):
                for i in range(side):
                    for j in range(side):
                        k = (i * side + j) * piece
                        own[term[c], o, k:k + piece, tn:] = down[
                            (o * side + i) * piece:(o * side + i + 1) * piece, (c * side + j) * lanes:(c * side + j + 1) * lanes
                        ]

    def weights_in(left, c):
        half = d // 2
        at = left[:, c * half:(c + 1) * half]
        own[term[c], 0, :, :tn] = t_dot(at, dgu_ref[:, :tn]).astype(BF16)
        own[term[c], 1, :, :tn] = t_dot(at, dgu_ref[:, tn:]).astype(BF16)

    @pl.when(n < 0)
    def _():
        slot = lax.rem(step, 2)

        def silu(c):
            rows = pl.ds(c * mc, mc)
            g, u = g_ref[slot, rows, :], u_ref[slot, rows, :]
            act_ref[rows, :] = (g * jax.nn.sigmoid(g) * u).astype(BF16)

        def down(c):
            rows = pl.ds(c * mc, mc)
            acc_ref[rows, :] += dot(act_ref[rows, :], wd_ref[0])

        gu(0, a0_ref, slot)
        for c in range(chunks):
            if c + 1 < chunks:
                gu(c + 1, a0_ref, slot)
            silu(c)
            if c > 0:
                down(c - 1)
        down(chunks - 1)
        for copy in put_gu(step):
            copy.start()

    @pl.when(n == -1)
    def _():
        @pl.loop(0, blocks)
        def _(i):
            rows = ds(i, block)
            y = acc_ref[rows, :].astype(BF16).astype(F32)
            h = (h_ref[rows, :].astype(F32) + y).astype(BF16)
            h_ref[rows, :] = h
            a_ref[rows, :] = norm_rows(h)
            acc_ref[rows, :] = jnp.zeros((block, d), F32)

    @pl.when((n >= 0) & (n < tiles))
    def _():
        def back(c):
            rows = pl.ds(c * mc, mc)
            acc_ref[rows, :] += dot_t(dgu_ref[rows, :tn], wg_ref[0]) + dot_t(dgu_ref[rows, tn:], wu_ref[0])

        gu(0, a_ref, 0)
        da(0, dy_ref)
        for c in range(1, chunks):
            gu(c, a_ref, 0)
            da(c, dy_ref)
            epi(c - 1, 0)
        back(0)
        epi(chunks - 1, 0)
        for c in range(1, chunks):
            back(c)
        exchange.tick(2 * n)
        weights_down(dy_ref)
        weights_in(a_ref, 0)
        weights_in(a_ref, 1)

    @pl.when((n >= tiles) & (n < 2 * tiles))
    def _():
        slot = lax.rem(n - tiles + 1, 2)
        for copy in get_gu(n - tiles):
            copy.wait()
        da(0, h_ref)
        for c in range(1, chunks):
            da(c, h_ref)
            epi(c - 1, slot)
        epi(chunks - 1, slot)
        weights_down(h_ref)
        weights_in(a0_ref, 0)
        weights_in(a0_ref, 1)

    @pl.when(n >= 0)
    def _():
        exchange.tick(jnp.where(n < tiles, 2 * n + 1, n + tiles))

    @pl.when(n == tiles - 1)
    def _():
        @pl.loop(0, blocks)
        def _(i):
            rows = ds(i, block)
            da = acc_ref[rows, :].astype(BF16).astype(F32)
            h = h_ref[rows, :].astype(F32)
            ms = jnp.mean(h * h, -1, keepdims=True) + 1e-6
            r = lax.rsqrt(ms)
            along = jnp.mean(da * h, -1, keepdims=True)
            dn = (r * (da - h * (along / ms))).astype(BF16).astype(F32)
            h_ref[rows, :] = (dy_ref[rows, :].astype(F32) + dn).astype(BF16)

    @pl.when(n == 2 * tiles - 1 + FINISH)
    def _():
        squares = Total(place, sums, vs, vr)
        value = jnp.full(factor_ref.shape, jnp.sum(sq_ref[...]), F32)
        for k in range(2):
            value = squares.over(k, value)
        factor_ref[...] = jnp.minimum(1.0, 0.5 * lax.rsqrt(value / count + 1e-30))


def layers(x, dy, wg, wu, wd, tn, side, gathered, count):
    t, d = x.shape
    ff = wg.shape[2]
    tiles = ff // tn
    piece, wide = d // (2 * side * side), tn + d // (2 * side)
    chunk = side * piece
    rows = side * chunk
    mc = t // 4
    hbm = pl.BlockSpec(memory_space=pl.ANY)
    layer = lambda n: jnp.where(n < tiles, 0, 1)
    tile = lambda n: jnp.where(n < tiles, n, jnp.minimum(n - tiles, tiles - 1))
    rest = (2 * tiles - gathered, 2, piece, wide)
    return pl.pallas_call(
        functools.partial(layers_kernel, mc=mc, side=side, tiles=tiles, gathered=gathered, count=count),
        grid=(3 * tiles + FINISH,),
        in_specs=[
            hbm,
            hbm,
            pl.BlockSpec((1, d, tn), lambda n: (layer(n), 0, tile(n))),
            pl.BlockSpec((1, d, tn), lambda n: (layer(n), 0, tile(n))),
            pl.BlockSpec((1, tn, d), lambda n: (
                jnp.where((n >= tiles) & (n < 2 * tiles), 1, 0), jnp.where(n < 3 * tiles, lax.rem(n, tiles), tiles - 1), 0
            )),
        ],
        out_specs=[
            hbm,
            pl.BlockSpec(rest, lambda n: (0, 0, 0, 0), **ONE),
            pl.BlockSpec((8, 128), lambda n: (0, 0), **ONE),
            hbm,
            hbm,
        ],
        out_shape=[
            jax.ShapeDtypeStruct((gathered, 2, 2, side * side, piece, wide), BF16),
            jax.ShapeDtypeStruct(rest, BF16),
            jax.ShapeDtypeStruct((8, 128), F32),
            jax.ShapeDtypeStruct((tiles, t, tn), F32),
            jax.ShapeDtypeStruct((tiles, t, tn), F32),
        ],
        scratch_shapes=[
            *[pltpu.VMEM((t, d), BF16)] * 4, pltpu.VMEM((t, d), F32),
            pltpu.VMEM((2, t, tn), F32), pltpu.VMEM((2, t, tn), F32), pltpu.VMEM((2, mc, tn), F32),
            pltpu.VMEM((t, tn), BF16), pltpu.VMEM((t, 2 * tn), BF16),
            pltpu.VMEM((OWN + 2, 2, rows, wide), BF16),
            pltpu.VMEM((MATE, 2, rows, wide), BF16),
            pltpu.VMEM((2, 2, (chunk + piece) * 3 // 2, wide), BF16),
            pltpu.VMEM((DEPTH, 2, 2, (chunk + piece) * 3 // 2, wide), BF16),
            pltpu.VMEM((DEPTH, 2, chunk, wide), F32),
            pltpu.VMEM((2 * tiles, 2, piece, wide), BF16),
            pltpu.VMEM((piece, wide), F32),
            pltpu.VMEM((2, 2 * side, 8, 128), F32),
            DMA((8,)), DMA, DMA((2, 2)), DMA((2, 2 * side)), DMA((2, 2 * side)), DMA((DEPTH, 2)),
            DMA((2,)), DMA((MATE,)),
            *[sem for name in range(6) for sem in (DMA, DMA((DEPTH,)))],
        ],
        compiler_params=pltpu.CompilerParams(
            vmem_limit_bytes=VLIM, dimension_semantics=("arbitrary",), collective_id=0, has_side_effects=True
        ),
        cost_estimate=pl.CostEstimate(flops=30 * t * d * ff, bytes_accessed=24 * d * ff, transcendentals=3 * t * ff),
        name="layers",
    )(x, dy, wg, wu, wd)[:3]


def adam_kernel(factor_ref, grad_ref, *refs, side, own):
    weights, moments, squares, new_w, new_m, new_v = (refs[i:i + 3] for i in [*range(0, 9, 3), *range(len(refs) - 9, len(refs), 3)])
    piece, wide = grad_ref.shape[-2:]
    tn = new_w[0].shape[2]
    lanes = wide - tn
    f = factor_ref[0, 0]

    def grad(c, o, i, j):
        if own:
            return grad_ref.at[0, c, o, i * side + j]
        return grad_ref.at[((i * side + j) if o == 0 else (j * side + i)) * 2 + c, 0, o]

    def step(k, at, g):
        g = g.astype(F32) * f
        m = 0.9 * moments[k][at] + 0.1 * g
        v = 0.95 * squares[k][at] + 0.05 * (g * g)
        w = weights[k][at].astype(F32)
        new_w[k][at] = (w - 0.02 * (m * lax.rsqrt(v + 1e-8) + 0.1 * w)).astype(BF16)
        new_m[k][at] = m
        new_v[k][at] = v

    for c in range(2):
        @pl.loop(0, side)
        def _(i):
            for j in range(side):
                for o in range(2):
                    step(o, (0, ds((c * side + i) * side + j, piece), slice(None)), grad(c, o, i, j)[:, :tn])
            for o in range(2):
                for j in range(side):
                    at = (0, ds(o * side + i, piece), slice((c * side + j) * lanes, (c * side + j + 1) * lanes))
                    step(2, at, grad(c, o, i, j)[:, tn:])


def adam(factor, grad, ws, ms, vs, so_far, tn, side, first, count):
    _, d, ff = ws[0].shape
    tiles = ff // tn
    at = lambda t: (1 - (t + first) // tiles, (t + first) % tiles)
    up = pl.BlockSpec((1, d, tn), lambda t: (at(t)[0], 0, at(t)[1]))
    down = pl.BlockSpec((1, tn, d), lambda t: (*at(t), 0))
    blocks = [up, up, down]
    own = not so_far
    size = sum(w.size for w in ws) * count // (2 * tiles)
    if own:
        grad_block = pl.BlockSpec((1, *grad.shape[1:]), lambda t: (t, 0, 0, 0, 0, 0))
    else:
        grad_block = pl.BlockSpec((grad.shape[0], 1, *grad.shape[2:]), lambda t: (0, t, 0, 0, 0))
    out = pl.pallas_call(
        functools.partial(adam_kernel, side=side, own=own),
        grid=(count,),
        in_specs=[
            pl.BlockSpec(factor.shape, lambda t: (0, 0), **ONE),
            grad_block,
            *blocks * 3,
            *[pl.BlockSpec(memory_space=pl.ANY)] * len(so_far),
        ],
        out_specs=blocks * 3,
        out_shape=[jax.ShapeDtypeStruct(a.shape, a.dtype) for a in (*ws, *ms, *vs)],
        input_output_aliases={11 + i: i for i in range(len(so_far))},
        compiler_params=pltpu.CompilerParams(vmem_limit_bytes=VLIM, dimension_semantics=("arbitrary",)),
        cost_estimate=pl.CostEstimate(flops=20 * size, bytes_accessed=22 * size, transcendentals=size),
        name="adam_own" if own else "adam_rest",
    )(factor, grad, *ws, *ms, *vs, *so_far)
    return tuple(out)


def solution(mesh):
    side = math.isqrt(mesh.shape["dp"] // 2)

    def step(x, dy, *arrays):
        ws, ms, vs = (arrays[i:i + 3] for i in (0, 3, 6))
        x, dy = x[0], dy[0]
        tn = x.shape[1] // side
        tiles = ws[0].shape[0] * ws[0].shape[2] // tn
        gathered = tiles * 6 // 10
        full, rest, factor = layers(x, dy, *ws, tn, side, gathered, sum(w.size for w in ws))
        rest = lax.all_gather(rest, "dp")
        new = adam(factor, full, ws, ms, vs, (), tn, side, 0, gathered)
        return adam(factor, rest, ws, ms, vs, new, tn, side, gathered, tiles - gathered)

    return jax.shard_map(
        step,
        mesh=mesh,
        in_specs=(P(("rep", "dp"), None, None),) * 2 + (P(None, None, None),) * 9,
        out_specs=(P("rep", None, None),) * 9,
        check_vma=False,
    )
```

```python
import functools
import math

import jax
import jax.numpy as jnp
from jax import lax
from jax.experimental import pallas as pl
from jax.experimental.pallas import tpu as pltpu
from jax.sharding import PartitionSpec as P

F32, BF16 = jnp.float32, jnp.bfloat16
MESH = pl.DeviceIdType.MESH
VLIM = 64 * 1024 * 1024 - 64 * 1024
DMA = pltpu.SemaphoreType.DMA
ONE = dict(pipeline_mode=pl.Buffered(1))


def dot(a, b):
    return jnp.dot(a, b, preferred_element_type=F32)


def dot_t(a, b):
    return lax.dot_general(a, b, (((1,), (1,)), ((), ())), preferred_element_type=F32)


def t_dot(a, b):
    return lax.dot_general(a, b, (((0,), (0,)), ((), ())), preferred_element_type=F32)


def ds(i, size):
    return pl.ds(pl.multiple_of(i * size, size), size)


def norm_rows(h):
    wide = h.astype(F32)
    scale = lax.rsqrt(jnp.mean(wide * wide, -1, keepdims=True) + 1e-6)
    return (wide * scale).astype(BF16)


class Place:
    def __init__(self, side):
        me = lax.axis_index("dp")
        self.core, chip = lax.rem(me, 2), lax.div(me, 2)
        x, y = lax.div(chip, side), lax.rem(chip, side)
        self.side = side
        at = lambda x, y, core: {"dp": (lax.rem(x + side, side) * side + lax.rem(y + side, side)) * 2 + core}
        self.partner = at(x, y, 1 - self.core)
        along_x = [at(x + k, y, self.core) for k in range(side)]
        along_y = [at(x, y + k, self.core) for k in range(side)]
        self.peers = [self.partner, along_x[1], along_x[-1], along_y[1], along_y[-1]]
        self.rings = [along_x, along_y]
        self.positions = [x * 2 + self.core, y]
        self.members = [[at(x + r // 2, y, lax.rem(self.core + r % 2, 2)) for r in range(2 * side)], along_y]
        ring = lambda p, r: (p, r[1], r[-1])
        self.first = [ring(x, along_x), ring(y, along_y)]
        self.second = [ring(y, along_y), ring(x, along_x)]

    def on(self, p, k):
        return lax.rem(p + k, self.side)


def remote(src, dst, send, recv, device):
    return pltpu.make_async_remote_copy(src_ref=src, dst_ref=dst, send_sem=send, recv_sem=recv, device_id=device, device_id_type=MESH)


def greet(peers):
    barrier = pltpu.get_barrier_semaphore()
    for peer in peers:
        pl.semaphore_signal(barrier, inc=1, device_id=peer, device_id_type=MESH)
    pl.semaphore_wait(barrier, len(peers))


OWN = 4
MATE = 4
DEPTH = 2
GROUP = 2
FINISH = 5


class Exchange:
    def __init__(self, tiles, gathered, place, buffers, semaphores, shard_ref, full_ref, rest_ref, sq_ref):
        self.tiles, self.gathered, self.place = tiles, gathered, place
        self.early = tiles // 2
        self.own, self.mate, self.out, self.inn, self.total = buffers
        self.sems = semaphores
        self.shard, self.full, self.rest, self.sq = shard_ref, full_ref, rest_ref, sq_ref
        self.rows = self.mate.shape[2] // place.side
        self.sub = self.rows // place.side
        half, small = self.rows // 2, self.sub // 2
        self.a, self.a2, self.b2, self.b = 0, half, half + small, half + small + self.sub

    def tile(self, tick):
        two = tick < 2 * self.early
        there = (tick >= 0) & (tick < self.tiles + self.early) & ((lax.rem(tick + 4 * self.tiles, 2) == 1) | jnp.logical_not(two))
        return jnp.where(two, lax.div(tick, 2), tick - self.early), there

    def neighbours(self):
        return [(axis, k, self.place.first[axis][1 + k]) for axis in range(2) for k in range(2)]

    def ring(self, tick, first, stop):
        slot = lax.rem(tick, DEPTH)
        send, recv = self.sems["ring"]
        rows = pl.ds(first, stop - first)
        return [
            remote(self.out.at[i, k, rows], self.inn.at[slot, i, k, rows], send, recv.at[slot], peer) for i, k, peer in self.neighbours()
        ]

    def ring_all(self, tick, first, stop, which):
        slot = lax.rem(tick, DEPTH)
        ref = self.inn.at[slot, :, :, pl.ds(first, stop - first)]
        send, recv = self.sems["ring"]
        return pltpu.make_async_copy(ref, ref, send if which == 0 else recv.at[slot])

    def in_parts(self, tick, what):
        end, middle, last = self.b + self.rows, 2 * self.early, self.tiles + self.early
        odd = lax.rem(tick + 2, 2) == 1
        for when, first, stop in (
            ((tick >= 0) & (tick < middle) & jnp.logical_not(odd), self.a, self.b2),
            ((tick >= 0) & (tick < middle) & odd, self.b2, end),
            ((tick >= middle) & (tick <= last), self.a, end),
            (tick == last + 1, self.a2, end),
            (tick == last + 2, self.a2, self.b),
            (tick == last + 3, self.b2, self.b),
        ):
            pl.when(when)(functools.partial(what, first, stop))

    def d2d(self, t):
        send, recv = self.sems["d2d"]
        two, mate = lax.rem(t, 2), lax.rem(t, MATE)
        return remote(self.own.at[OWN + two], self.mate.at[mate], send.at[two], recv.at[mate], self.place.partner)

    def chip(self, t, o, first, count):
        at = pl.ds(pl.multiple_of(first, count), count)
        return self.own[lax.rem(t, OWN), o, at, :].astype(F32) + self.mate[lax.rem(t, MATE), o, at, :].astype(F32)

    def sum_a(self, t, slot):
        half = self.rows // 2
        for o in range(2):
            chunk = self.place.on(self.place.first[o][0], 2)
            for i in range(0, self.rows, self.sub):
                at = self.a + i % half
                self.out[o, i // half, at:at + self.sub, :] = self.chip(t, o, chunk * self.rows + i, self.sub).astype(BF16)

    def sum_b(self, t, slot, k):
        half, side = self.rows // 2, self.place.side
        for o in range(2):
            chunk = self.place.on(self.place.first[o][0], (1, side - 1)[k])
            for i in range(0, self.rows, self.sub):
                x = self.chip(t, o, chunk * self.rows + i, self.sub)
                if i // half == k:
                    at = self.a + i % half
                    x = x + self.inn[slot, o, k, at:at + self.sub, :].astype(F32)
                at = self.b + i
                self.out[o, k, at:at + self.sub, :] = x.astype(BF16)

    def sum_a2(self, t, slot, o):
        keep, half = lax.rem(t, DEPTH), self.sub // 2
        chunk = self.place.first[o][0]
        for i in range(0, self.rows, self.sub):
            x = self.chip(t, o, chunk * self.rows + i, self.sub)
            at = self.b + i
            for k in range(2):
                x = x + self.inn[slot, o, k, at:at + self.sub, :].astype(F32)
            self.total[keep, o, i:i + self.sub, :] = x
        far = self.place.on(self.place.second[o][0], 2)
        for k in range(2):
            x = self.total[keep, o, pl.ds(pl.multiple_of(far * self.sub + k * half, half), half), :]
            self.out[1 - o, k, self.a2:self.a2 + half, :] = x.astype(BF16)

    def sum_b2(self, t, slot):
        keep, half, side = lax.rem(t, DEPTH), self.sub // 2, self.place.side
        for o in range(2):
            for k in range(2):
                chunk = self.place.on(self.place.second[o][0], (1, side - 1)[k])
                for i in range(2):
                    x = self.total[keep, o, pl.ds(pl.multiple_of(chunk * self.sub + i * half, half), half), :]
                    if i == k:
                        x = x + self.inn[slot, 1 - o, k, self.a2:self.a2 + half, :].astype(F32)
                    at = self.b2 + i * half
                    self.out[1 - o, k, at:at + half, :] = x.astype(BF16)

    def finish(self, t, slot):
        keep = lax.rem(t, DEPTH)
        for o in range(2):
            x = self.total[keep, o, ds(self.place.second[o][0], self.sub), :]
            for k in range(2):
                x = x + self.inn[slot, 1 - o, k, self.b2:self.b2 + self.sub, :].astype(F32)
            g = x.astype(BF16)
            self.shard[t, o] = g
            g = g.astype(F32)
            self.sq[...] += g * g

        @pl.when(t >= self.gathered)
        def _():
            self.rest[t - self.gathered] = self.shard[t]

    def tiles_of(self, q):
        return pl.ds(q * GROUP, GROUP)

    def cell(self, q, o, step):
        p, at = self.place.first[o][0], self.place.second[o][0]
        return self.full.at[self.tiles_of(q), self.place.core, o, p * self.place.side + self.place.on(at, step)]

    def line(self, q, o, step, first, size):
        i = self.place.on(self.place.first[o][0], step)
        return self.full.at[self.tiles_of(q), self.place.core, o, pl.ds(i * self.place.side + first, size)]

    def keep(self, q):
        return [
            pltpu.make_async_copy(self.shard.at[self.tiles_of(q), o], self.cell(q, o, 0), self.sems["keep"].at[lax.rem(q, DEPTH), o])
            for o in range(2)
        ]

    def gather(self, name, q):
        send, recv = self.sems[name]
        recv = recv.at[lax.rem(q, DEPTH)]
        side, half = self.place.side, self.sub // 2
        if name == "h":
            both = self.full.at[self.tiles_of(q), self.place.core]
            return [remote(both, both, send, recv, self.place.partner)]
        copies = []
        for o in range(2):
            for k in range(2):
                back = (side - 1, 1)[k]
                if name == "d":
                    src, dst = self.shard.at[self.tiles_of(q), o], self.cell(q, o, 0)
                elif name == "e":
                    p, at = self.place.first[o][0], self.place.second[o][0]
                    src = dst = self.full.at[
                        self.tiles_of(q), self.place.core, o, p * side + self.place.on(at, back), pl.ds(k * half, half)
                    ]
                elif name == "f":
                    src = dst = self.line(q, o, 0, 0, side)
                else:
                    src = dst = self.line(q, o, back, k * side // 2, side // 2)
                axis = self.place.second if name in "de" else self.place.first
                copies.append(remote(src, dst, send, recv, axis[o][1 + k]))
        return copies

    def gather_all(self, name, q, which):
        send, recv = self.sems[name]
        side = self.place.side
        if name == "d":
            ref = self.shard.at[pl.ds(0, 2 * GROUP)]
        elif name == "e":
            ref = self.shard.at[pl.ds(0, GROUP)]
        elif name == "f":
            ref = self.full.at[pl.ds(0, GROUP), 0, 0]
        elif name == "g":
            ref = self.full.at[pl.ds(0, GROUP), 0, 0, pl.ds(0, side * side // 2)]
        else:
            ref = self.full.at[pl.ds(0, GROUP), 0]
        return pltpu.make_async_copy(ref, ref, send if which == 0 else recv.at[lax.rem(q, DEPTH)])

    def gather_step(self, tick, i, before, after):
        t, there = self.tile(tick - FINISH - 1 - i)
        q = lax.div(t, GROUP)

        @pl.when(there & (t < self.gathered) & (lax.rem(t, GROUP) == GROUP - 1))
        def _():
            if before:
                self.gather_all(before, q, 1).wait()
                self.gather_all(before, q, 0).wait()
            if after == "f":
                for copy in self.keep(q):
                    copy.wait()
            if after:
                for copy in self.gather(after, q):
                    copy.start()
            if after == "d":
                for copy in self.keep(q):
                    copy.start()

    def tick(self, tick):
        def ring_wait(first, stop):
            self.ring_all(tick - 1, first, stop, 1).wait()
            self.ring_all(tick - 1, first, stop, 0).wait()

        def ring_start(first, stop):
            for copy in self.ring(tick, first, stop):
                copy.start()

        slot = lax.rem(tick + 1, DEPTH)
        self.in_parts(tick - 1, ring_wait)

        t5, there = self.tile(tick - FINISH)
        pl.when(there)(lambda: self.finish(t5, slot))

        t, there = self.tile(tick - 2)

        @pl.when(there)
        def _():
            self.sum_b(t, slot, 0)
            self.sum_b(t, slot, 1)

        t1, there = self.tile(tick - 1)

        @pl.when(there)
        def _():
            self.d2d(t1).wait_recv()
            self.d2d(t1).wait_send()
            self.sum_a(t1, slot)

        t3, there = self.tile(tick - 3)

        @pl.when(there)
        def _():
            self.sum_a2(t3, slot, 0)
            self.sum_a2(t3, slot, 1)

        t4, there = self.tile(tick - 4)

        @pl.when(there)
        def _():
            self.sum_b2(t4, slot)

        t0, there = self.tile(tick)

        @pl.when(there)
        def _():
            self.d2d(t0).start()

        self.in_parts(tick, ring_start)

        stages = ("d", "e", "f", "g", "h", "")
        for i in reversed(range(6)):
            self.gather_step(tick, i, stages[i - 1] if i else "", stages[i])


class Total:
    def __init__(self, place, sums, send, recv):
        self.place, self.sums, self.send, self.recv = place, sums, send, recv

    def over(self, k, value):
        members, me = self.place.members[k], self.place.positions[k]
        self.sums[k, me] = value
        here = self.sums.at[k, me]
        copies = [remote(here, here, self.send.at[k, i], self.recv.at[k, i], peer) for i, peer in enumerate(members) if i]
        for copy in copies:
            copy.start()
        for copy in copies:
            copy.wait()
        value = self.sums[k, 0]
        for i in range(1, len(members)):
            value = value + self.sums[k, i]
        return value


def gates(g, u, dact):
    s = jax.nn.sigmoid(g)
    silu = g * s
    act = (silu * u).astype(BF16)
    dup = (dact * silu).astype(BF16)
    dgate = (dact * u * (s + silu * (1.0 - s))).astype(BF16)
    return act, dgate, dup


def layers_kernel(x_hbm, dy_hbm, wg_hbm, wu_hbm, wd_hbm, full_ref, rest_ref, factor_ref, gate_hbm, up_hbm,
                  wg_ref, wu_ref, wd_ref, dy_ref, h_ref, a_ref, a0_ref, acc_ref, g_ref, u_ref, dact_ref, act_ref, dgu_ref,
                  own, mate, out, inn, total, shard_ref, sq_ref, sums,
                  w_sem, x_sem, dy_sem, gu_sem, vs, vr, keep_sem, *pairs, mc, side, tiles, gathered, count):
    tokens, d = h_ref.shape
    tn = wg_ref.shape[2]
    chunks, blocks = tokens // mc, x_sem.shape[0]
    block = tokens // blocks
    place = Place(side)
    piece = d // (2 * side * side)
    sems = {name: pairs[2 * i:2 * i + 2] for i, name in enumerate(("d2d", "ring", "d", "e", "f", "g", "h"))}
    sems["keep"] = keep_sem
    exchange = Exchange(2 * tiles, gathered, place, (own, mate, out, inn, total), sems, shard_ref, full_ref, rest_ref, sq_ref)

    def load_x(i):
        rows = ds(i, block)
        return pltpu.make_async_copy(x_hbm.at[rows], h_ref.at[rows], x_sem.at[i])

    def load_dy():
        return pltpu.make_async_copy(dy_hbm, dy_ref, dy_sem)

    def load_in(layer, t):
        slot = lax.rem(t, 2)
        return [
            pltpu.make_async_copy(wg_hbm.at[layer, :, ds(t, tn)], wg_ref.at[slot], w_sem.at[slot, 0]),
            pltpu.make_async_copy(wu_hbm.at[layer, :, ds(t, tn)], wu_ref.at[slot], w_sem.at[slot, 1]),
        ]

    def load_down(layer, t):
        slot = lax.rem(t, 2)
        return [pltpu.make_async_copy(wd_hbm.at[layer, ds(t, tn)], wd_ref.at[slot], w_sem.at[slot, 2])]

    def put_gu(t):
        slot = lax.rem(t, 2)
        return [
            pltpu.make_async_copy(g_ref.at[slot], gate_hbm.at[t], gu_sem.at[slot, 0]),
            pltpu.make_async_copy(u_ref.at[slot], up_hbm.at[t], gu_sem.at[slot, 1]),
        ]

    def get_gu(t):
        slot = lax.rem(t + 1, 2)
        return [
            pltpu.make_async_copy(gate_hbm.at[t], g_ref.at[slot], gu_sem.at[slot, 0]),
            pltpu.make_async_copy(up_hbm.at[t], u_ref.at[slot], gu_sem.at[slot, 1]),
        ]

    def start(copies):
        for copy in copies:
            copy.start()

    def wait(copies):
        for copy in copies:
            copy.wait()

    def ahead(layer, t, what):
        for load in what:
            pl.when(t + 1 < tiles)(lambda load=load: start(load(layer, t + 1)))
            wait(load(layer, t))

    def gu(c, t, a, slot):
        rows = pl.ds(c * mc, mc)
        a = a[rows, :]
        g_ref[slot, rows, :] = dot(a, wg_ref[lax.rem(t, 2)])
        u_ref[slot, rows, :] = dot(a, wu_ref[lax.rem(t, 2)])

    def da(c, t, right):
        dact_ref[c % 2] = dot_t(right[pl.ds(c * mc, mc), :], wd_ref[lax.rem(t, 2)])

    def epi(c, slot):
        rows = pl.ds(c * mc, mc)
        dact = dact_ref[c % 2].astype(BF16).astype(F32)
        act, dgate, dup = gates(g_ref[slot, rows, :], u_ref[slot, rows, :], dact)
        act_ref[rows, :] = act
        dgu_ref[rows, :tn] = dgate
        dgu_ref[rows, tn:] = dup

    def terms(n, left, right):
        term = [jnp.where(place.core == c, lax.rem(n, OWN), OWN + lax.rem(n, 2)) for c in range(2)]
        lanes, half = d // (2 * side), d // 2
        down = t_dot(act_ref[...], right[...]).astype(BF16)
        for o in range(2):
            for c in range(2):
                for i in range(side):
                    for j in range(side):
                        k = (i * side + j) * piece
                        own[term[c], o, k:k + piece, tn:] = down[
                            (o * side + i) * piece:(o * side + i + 1) * piece, (c * side + j) * lanes:(c * side + j + 1) * lanes
                        ]
        for c in range(2):
            at = left[:, c * half:(c + 1) * half]
            own[term[c], 0, :, :tn] = t_dot(at, dgu_ref[:, :tn]).astype(BF16)
            own[term[c], 1, :, :tn] = t_dot(at, dgu_ref[:, tn:]).astype(BF16)

    for i in range(blocks):
        load_x(i).start()
    start(load_in(0, 0) + load_down(0, 0))
    load_dy().start()
    greet([*place.members[0][1:], *place.members[1][1:]])
    sq_ref[...] = jnp.zeros_like(sq_ref)

    @pl.loop(0, blocks)
    def _(i):
        rows = ds(i, block)
        load_x(i).wait()
        a0_ref[rows, :] = norm_rows(h_ref[rows, :])
        acc_ref[rows, :] = jnp.zeros((block, d), F32)

    @pl.loop(0, tiles)
    def _(t):
        slot = lax.rem(t, 2)
        pl.when(t >= 2)(lambda: wait(put_gu(t - 2)))
        ahead(0, t, (load_in, load_down))

        def silu(c):
            rows = pl.ds(c * mc, mc)
            g, u = g_ref[slot, rows, :], u_ref[slot, rows, :]
            act_ref[rows, :] = (g * jax.nn.sigmoid(g) * u).astype(BF16)

        def down(c):
            rows = pl.ds(c * mc, mc)
            acc_ref[rows, :] += dot(act_ref[rows, :], wd_ref[slot])

        gu(0, t, a0_ref, slot)
        for c in range(chunks):
            if c + 1 < chunks:
                gu(c + 1, t, a0_ref, slot)
            silu(c)
            if c > 0:
                down(c - 1)
        down(chunks - 1)
        start(put_gu(t))

    start(load_in(1, 0) + load_down(1, 0))

    @pl.loop(0, blocks)
    def _(i):
        rows = ds(i, block)
        y = acc_ref[rows, :].astype(BF16).astype(F32)
        h = (h_ref[rows, :].astype(F32) + y).astype(BF16)
        h_ref[rows, :] = h
        a_ref[rows, :] = norm_rows(h)
        acc_ref[rows, :] = jnp.zeros((block, d), F32)

    wait(put_gu(tiles - 2) + put_gu(tiles - 1) + [load_dy()])
    start(get_gu(0))

    @pl.loop(0, tiles)
    def _(n):
        ahead(1, n, (load_in, load_down))

        def back(c):
            rows = pl.ds(c * mc, mc)
            slot = lax.rem(n, 2)
            acc_ref[rows, :] += dot_t(dgu_ref[rows, :tn], wg_ref[slot]) + dot_t(dgu_ref[rows, tn:], wu_ref[slot])

        gu(0, n, a_ref, 0)
        da(0, n, dy_ref)
        for c in range(1, chunks):
            gu(c, n, a_ref, 0)
            da(c, n, dy_ref)
            epi(c - 1, 0)
        back(0)
        epi(chunks - 1, 0)
        for c in range(1, chunks):
            back(c)
        exchange.tick(2 * n)
        terms(n, a_ref, dy_ref)
        exchange.tick(2 * n + 1)

    start(load_down(0, 0))

    @pl.loop(0, blocks)
    def _(i):
        rows = ds(i, block)
        da = acc_ref[rows, :].astype(BF16).astype(F32)
        h = h_ref[rows, :].astype(F32)
        ms = jnp.mean(h * h, -1, keepdims=True) + 1e-6
        r = lax.rsqrt(ms)
        along = jnp.mean(da * h, -1, keepdims=True)
        dn = (r * (da - h * (along / ms))).astype(BF16).astype(F32)
        h_ref[rows, :] = (dy_ref[rows, :].astype(F32) + dn).astype(BF16)

    @pl.loop(0, tiles)
    def _(t):
        slot = lax.rem(t + 1, 2)
        ahead(0, t, (load_down,))
        pl.when(t + 1 < tiles)(lambda: start(get_gu(t + 1)))
        wait(get_gu(t))
        da(0, t, h_ref)
        for c in range(1, chunks):
            da(c, t, h_ref)
            epi(c - 1, slot)
        epi(chunks - 1, slot)
        terms(tiles + t, a0_ref, h_ref)
        exchange.tick(2 * tiles + t)

    @pl.loop(0, FINISH)
    def _(i):
        exchange.tick(3 * tiles + i)

    squares = Total(place, sums, vs, vr)
    value = jnp.full(factor_ref.shape, jnp.sum(sq_ref[...]), F32)
    for k in range(2):
        value = squares.over(k, value)
    factor_ref[...] = jnp.minimum(1.0, 0.5 * lax.rsqrt(value / count + 1e-30))


def layers(x, dy, wg, wu, wd, tn, side, gathered, count):
    t, d = x.shape
    ff = wg.shape[2]
    tiles = ff // tn
    piece, wide = d // (2 * side * side), tn + d // (2 * side)
    chunk = side * piece
    rows = side * chunk
    mc = t // 4
    hbm = pl.BlockSpec(memory_space=pl.ANY)
    rest = (2 * tiles - gathered, 2, piece, wide)
    return pl.pallas_call(
        functools.partial(layers_kernel, mc=mc, side=side, tiles=tiles, gathered=gathered, count=count),
        in_specs=[hbm] * 5,
        out_specs=[hbm, pl.BlockSpec(memory_space=pltpu.VMEM), pl.BlockSpec(memory_space=pltpu.VMEM), hbm, hbm],
        out_shape=[
            jax.ShapeDtypeStruct((gathered, 2, 2, side * side, piece, wide), BF16),
            jax.ShapeDtypeStruct(rest, BF16),
            jax.ShapeDtypeStruct((8, 128), F32),
            jax.ShapeDtypeStruct((tiles, t, tn), F32),
            jax.ShapeDtypeStruct((tiles, t, tn), F32),
        ],
        scratch_shapes=[
            pltpu.VMEM((2, d, tn), BF16), pltpu.VMEM((2, d, tn), BF16), pltpu.VMEM((2, tn, d), BF16),
            *[pltpu.VMEM((t, d), BF16)] * 4, pltpu.VMEM((t, d), F32),
            pltpu.VMEM((2, t, tn), F32), pltpu.VMEM((2, t, tn), F32), pltpu.VMEM((2, mc, tn), F32),
            pltpu.VMEM((t, tn), BF16), pltpu.VMEM((t, 2 * tn), BF16),
            pltpu.VMEM((OWN + 2, 2, rows, wide), BF16),
            pltpu.VMEM((MATE, 2, rows, wide), BF16),
            pltpu.VMEM((2, 2, (chunk + piece) * 3 // 2, wide), BF16),
            pltpu.VMEM((DEPTH, 2, 2, (chunk + piece) * 3 // 2, wide), BF16),
            pltpu.VMEM((DEPTH, 2, chunk, wide), F32),
            pltpu.VMEM((2 * tiles, 2, piece, wide), BF16),
            pltpu.VMEM((piece, wide), F32),
            pltpu.VMEM((2, 2 * side, 8, 128), F32),
            DMA((2, 3)), DMA((8,)), DMA, DMA((2, 2)), DMA((2, 2 * side)), DMA((2, 2 * side)), DMA((DEPTH, 2)),
            DMA((2,)), DMA((MATE,)),
            *[sem for name in range(6) for sem in (DMA, DMA((DEPTH,)))],
        ],
        compiler_params=pltpu.CompilerParams(
            vmem_limit_bytes=VLIM, collective_id=0, has_side_effects=True
        ),
        cost_estimate=pl.CostEstimate(flops=30 * t * d * ff, bytes_accessed=24 * d * ff, transcendentals=3 * t * ff),
        name="layers",
    )(x, dy, wg, wu, wd)[:3]


def adam_kernel(factor_ref, grad_ref, *refs, side, own):
    weights, moments, squares, new_w, new_m, new_v = (refs[i:i + 3] for i in [*range(0, 9, 3), *range(len(refs) - 9, len(refs), 3)])
    piece, wide = grad_ref.shape[-2:]
    tn = new_w[0].shape[2]
    lanes = wide - tn
    f = factor_ref[0, 0]

    def grad(c, o, i, j):
        if own:
            return grad_ref.at[0, c, o, i * side + j]
        return grad_ref.at[((i * side + j) if o == 0 else (j * side + i)) * 2 + c, 0, o]

    def step(k, at, g):
        g = g.astype(F32) * f
        m = 0.9 * moments[k][at] + 0.1 * g
        v = 0.95 * squares[k][at] + 0.05 * (g * g)
        w = weights[k][at].astype(F32)
        new_w[k][at] = (w - 0.02 * (m * lax.rsqrt(v + 1e-8) + 0.1 * w)).astype(BF16)
        new_m[k][at] = m
        new_v[k][at] = v

    for c in range(2):
        @pl.loop(0, side)
        def _(i):
            for j in range(side):
                for o in range(2):
                    step(o, (0, ds((c * side + i) * side + j, piece), slice(None)), grad(c, o, i, j)[:, :tn])
            for o in range(2):
                for j in range(side):
                    at = (0, ds(o * side + i, piece), slice((c * side + j) * lanes, (c * side + j + 1) * lanes))
                    step(2, at, grad(c, o, i, j)[:, tn:])


def adam(factor, grad, ws, ms, vs, so_far, tn, side, first, count):
    _, d, ff = ws[0].shape
    tiles = ff // tn
    at = lambda t: (1 - (t + first) // tiles, (t + first) % tiles)
    up = pl.BlockSpec((1, d, tn), lambda t: (at(t)[0], 0, at(t)[1]))
    down = pl.BlockSpec((1, tn, d), lambda t: (*at(t), 0))
    blocks = [up, up, down]
    own = not so_far
    size = sum(w.size for w in ws) * count // (2 * tiles)
    if own:
        grad_block = pl.BlockSpec((1, *grad.shape[1:]), lambda t: (t, 0, 0, 0, 0, 0))
    else:
        grad_block = pl.BlockSpec((grad.shape[0], 1, *grad.shape[2:]), lambda t: (0, t, 0, 0, 0))
    out = pl.pallas_call(
        functools.partial(adam_kernel, side=side, own=own),
        grid=(count,),
        in_specs=[
            pl.BlockSpec(factor.shape, lambda t: (0, 0), **ONE),
            grad_block,
            *blocks * 3,
            *[pl.BlockSpec(memory_space=pl.ANY)] * len(so_far),
        ],
        out_specs=blocks * 3,
        out_shape=[jax.ShapeDtypeStruct(a.shape, a.dtype) for a in (*ws, *ms, *vs)],
        input_output_aliases={11 + i: i for i in range(len(so_far))},
        compiler_params=pltpu.CompilerParams(vmem_limit_bytes=VLIM, dimension_semantics=("arbitrary",)),
        cost_estimate=pl.CostEstimate(flops=20 * size, bytes_accessed=22 * size, transcendentals=size),
        name="adam_own" if own else "adam_rest",
    )(factor, grad, *ws, *ms, *vs, *so_far)
    return tuple(out)


def solution(mesh):
    side = math.isqrt(mesh.shape["dp"] // 2)

    def step(x, dy, *arrays):
        ws, ms, vs = (arrays[i:i + 3] for i in (0, 3, 6))
        x, dy = x[0], dy[0]
        tn = x.shape[1] // side
        tiles = ws[0].shape[0] * ws[0].shape[2] // tn
        gathered = tiles * 6 // 10
        full, rest, factor = layers(x, dy, *ws, tn, side, gathered, sum(w.size for w in ws))
        rest = lax.all_gather(rest, "dp")
        new = adam(factor, full, ws, ms, vs, (), tn, side, 0, gathered)
        return adam(factor, rest, ws, ms, vs, new, tn, side, gathered, tiles - gathered)

    return jax.shard_map(
        step,
        mesh=mesh,
        in_specs=(P(("rep", "dp"), None, None),) * 2 + (P(None, None, None),) * 9,
        out_specs=(P("rep", None, None),) * 9,
        check_vma=False,
    )
```

```python
import functools
import math

import jax
import jax.numpy as jnp
from jax import lax
from jax.experimental import pallas as pl
from jax.experimental.pallas import tpu as pltpu
from jax.sharding import PartitionSpec as P

F32, BF16 = jnp.float32, jnp.bfloat16
MESH = pl.DeviceIdType.MESH
VLIM = 64 * 1024 * 1024 - 64 * 1024
DMA = pltpu.SemaphoreType.DMA
ONE = dict(pipeline_mode=pl.Buffered(1))


def dot(a, b):
    return jnp.dot(a, b, preferred_element_type=F32)


def dot_t(a, b):
    return lax.dot_general(a, b, (((1,), (1,)), ((), ())), preferred_element_type=F32)


def t_dot(a, b):
    return lax.dot_general(a, b, (((0,), (0,)), ((), ())), preferred_element_type=F32)


def ds(i, size):
    return pl.ds(pl.multiple_of(i * size, size), size)


def norm_rows(h):
    wide = h.astype(F32)
    scale = lax.rsqrt(jnp.mean(wide * wide, -1, keepdims=True) + 1e-6)
    return (wide * scale).astype(BF16)


class Place:
    def __init__(self, side):
        me = lax.axis_index("dp")
        self.core, chip = lax.rem(me, 2), lax.div(me, 2)
        x, y = lax.div(chip, side), lax.rem(chip, side)
        self.side = side
        at = lambda x, y, core: {"dp": (lax.rem(x + side, side) * side + lax.rem(y + side, side)) * 2 + core}
        self.partner = at(x, y, 1 - self.core)
        along_x = [at(x + k, y, self.core) for k in range(side)]
        along_y = [at(x, y + k, self.core) for k in range(side)]
        self.peers = [self.partner, along_x[1], along_x[-1], along_y[1], along_y[-1]]
        self.rings = [along_x, along_y]
        self.positions = [x * 2 + self.core, y]
        self.members = [[at(x + r // 2, y, lax.rem(self.core + r % 2, 2)) for r in range(2 * side)], along_y]
        ring = lambda p, r: (p, r[1], r[-1])
        self.first = [ring(x, along_x), ring(y, along_y)]
        self.second = [ring(y, along_y), ring(x, along_x)]

    def on(self, p, k):
        return lax.rem(p + k, self.side)


def remote(src, dst, send, recv, device):
    return pltpu.make_async_remote_copy(src_ref=src, dst_ref=dst, send_sem=send, recv_sem=recv, device_id=device, device_id_type=MESH)


def greet(peers):
    barrier = pltpu.get_barrier_semaphore()
    for peer in peers:
        pl.semaphore_signal(barrier, inc=1, device_id=peer, device_id_type=MESH)
    pl.semaphore_wait(barrier, len(peers))


OWN = 4
MATE = 6
DEPTH = 2
GROUP = 2
FINISH = 5


class Exchange:
    def __init__(self, tiles, gathered, place, buffers, semaphores, shard_ref, full_ref, rest_ref, sq_ref):
        self.tiles, self.gathered, self.place = tiles, gathered, place
        self.early = tiles // 2
        self.own, self.mate, self.out, self.inn, self.out2, self.inn2, self.total = buffers
        self.sems = semaphores
        self.shard, self.full, self.rest, self.sq = shard_ref, full_ref, rest_ref, sq_ref
        self.rows = self.mate.shape[2] // place.side
        self.sub = self.rows // place.side
        self.b, self.b2 = self.rows // 2, self.sub // 2

    def tile(self, tick):
        two = tick < 2 * self.early
        there = (tick >= 0) & (tick < self.tiles + self.early) & ((lax.rem(tick + 4 * self.tiles, 2) == 1) | jnp.logical_not(two))
        return jnp.where(two, lax.div(tick, 2), tick - self.early), there

    def ring(self, tick, o, one, two):
        slot = lax.rem(tick, DEPTH)
        copies = []
        for rows, axis, out, inn, name in ((one, self.place.first, self.out, self.inn, 0), (two, self.place.second, self.out2, self.inn2, 1)):
            if rows:
                send, recv = self.sems["ring"]
                at = pl.ds(rows[0], rows[1] - rows[0])
                copies += [
                    remote(out.at[o, k, at], inn.at[slot, o, k, at], send.at[o, name], recv.at[slot, o, name], axis[o][1 + k])
                    for k in range(2)
                ]
        return copies

    def ring_wait(self, tick, o, one, two):
        slot = lax.rem(tick, DEPTH)
        send, recv = self.sems["ring"]
        for rows, inn, name in ((one, self.inn, 0), (two, self.inn2, 1)):
            if rows:
                ref = inn.at[slot, o, :, pl.ds(rows[0], rows[1] - rows[0])]
                pltpu.make_async_copy(ref, ref, recv.at[slot, o, name]).wait()
                pltpu.make_async_copy(ref, ref, send.at[o, name]).wait()

    def in_parts(self, tick, what):
        middle, last = 2 * self.early, self.tiles + self.early
        end, end2 = self.b + self.rows, self.b2 + self.sub
        odd = lax.rem(tick + 2, 2) == 1
        for when, one, two in (
            ((tick >= 0) & (tick < middle) & jnp.logical_not(odd), (0, self.b), (0, self.b2)),
            ((tick >= 0) & (tick < middle) & odd, (self.b, end), (self.b2, end2)),
            ((tick >= middle) & (tick <= last), (0, end), (0, end2)),
            (tick == last + 1, (self.b, end), (0, end2)),
            (tick == last + 2, None, (0, end2)),
            (tick == last + 3, None, (self.b2, end2)),
        ):
            pl.when(when)(functools.partial(what, one, two))

    def d2d(self, t):
        send, recv = self.sems["d2d"]
        two, mate = lax.rem(t, 2), lax.rem(t, MATE)
        return remote(self.own.at[OWN + two], self.mate.at[mate], send.at[two], recv.at[mate], self.place.partner)

    def chip(self, t, o, first, count):
        at = pl.ds(pl.multiple_of(first, count), count)
        return self.own[lax.rem(t, OWN), o, at, :].astype(F32) + self.mate[lax.rem(t, MATE), o, at, :].astype(F32)

    def sum_a(self, t, o):
        chunk = self.place.on(self.place.first[o][0], 2)
        for i in range(0, self.rows, self.sub):
            at = i % self.b
            self.out[o, i // self.b, at:at + self.sub, :] = self.chip(t, o, chunk * self.rows + i, self.sub).astype(BF16)

    def sum_b(self, t, slot, o):
        for k in range(2):
            chunk = self.place.on(self.place.first[o][0], (1, self.place.side - 1)[k])
            for i in range(0, self.rows, self.sub):
                x = self.chip(t, o, chunk * self.rows + i, self.sub)
                if i // self.b == k:
                    at = i % self.b
                    x = x + self.inn[slot, o, k, at:at + self.sub, :].astype(F32)
                self.out[o, k, self.b + i:self.b + i + self.sub, :] = x.astype(BF16)

    def sum_a2(self, t, slot, o):
        keep, half = lax.rem(t, DEPTH), self.b2
        chunk = self.place.first[o][0]
        for i in range(0, self.rows, self.sub):
            x = self.chip(t, o, chunk * self.rows + i, self.sub)
            for k in range(2):
                x = x + self.inn[slot, o, k, self.b + i:self.b + i + self.sub, :].astype(F32)
            self.total[keep, o, i:i + self.sub, :] = x
        far = self.place.on(self.place.second[o][0], 2)
        for k in range(2):
            x = self.total[keep, o, pl.ds(pl.multiple_of(far * self.sub + k * half, half), half), :]
            self.out2[o, k, :half, :] = x.astype(BF16)

    def sum_b2(self, t, slot, o):
        keep, half = lax.rem(t, DEPTH), self.b2
        for k in range(2):
            chunk = self.place.on(self.place.second[o][0], (1, self.place.side - 1)[k])
            for i in range(2):
                x = self.total[keep, o, pl.ds(pl.multiple_of(chunk * self.sub + i * half, half), half), :]
                if i == k:
                    x = x + self.inn2[slot, o, k, :half, :].astype(F32)
                self.out2[o, k, half + i * half:2 * half + i * half, :] = x.astype(BF16)

    def finish(self, t, slot, o):
        x = self.total[lax.rem(t, DEPTH), o, ds(self.place.second[o][0], self.sub), :]
        for k in range(2):
            x = x + self.inn2[slot, o, k, self.b2:, :].astype(F32)
        g = x.astype(BF16)
        self.shard[t, o] = g

        @pl.when(t >= self.gathered)
        def _():
            self.rest[t - self.gathered, o] = g

        g = g.astype(F32)
        self.sq[...] += g * g

    def tiles_of(self, q):
        return pl.ds(q * GROUP, GROUP)

    def cell(self, q, o, step):
        p, at = self.place.first[o][0], self.place.second[o][0]
        return self.full.at[self.tiles_of(q), self.place.core, o, p * self.place.side + self.place.on(at, step)]

    def line(self, q, o, step, first, size):
        i = self.place.on(self.place.first[o][0], step)
        return self.full.at[self.tiles_of(q), self.place.core, o, pl.ds(i * self.place.side + first, size)]

    def keep(self, q):
        return [
            pltpu.make_async_copy(self.shard.at[self.tiles_of(q), o], self.cell(q, o, 0), self.sems["keep"].at[lax.rem(q, DEPTH), o])
            for o in range(2)
        ]

    def gather(self, name, q):
        send, recv = self.sems[name]
        recv = recv.at[lax.rem(q, DEPTH)]
        side, half = self.place.side, self.sub // 2
        if name == "h":
            both = self.full.at[self.tiles_of(q), self.place.core]
            return [remote(both, both, send, recv, self.place.partner)]
        copies = []
        for o in range(2):
            for k in range(2):
                back = (side - 1, 1)[k]
                if name == "d":
                    src, dst = self.shard.at[self.tiles_of(q), o], self.cell(q, o, 0)
                elif name == "e":
                    p, at = self.place.first[o][0], self.place.second[o][0]
                    src = dst = self.full.at[
                        self.tiles_of(q), self.place.core, o, p * side + self.place.on(at, back), pl.ds(k * half, half)
                    ]
                elif name == "f":
                    src = dst = self.line(q, o, 0, 0, side)
                else:
                    src = dst = self.line(q, o, back, k * side // 2, side // 2)
                axis = self.place.second if name in "de" else self.place.first
                copies.append(remote(src, dst, send, recv, axis[o][1 + k]))
        return copies

    def gather_all(self, name, q, which):
        send, recv = self.sems[name]
        side = self.place.side
        if name == "d":
            ref = self.shard.at[pl.ds(0, 2 * GROUP)]
        elif name == "e":
            ref = self.shard.at[pl.ds(0, GROUP)]
        elif name == "f":
            ref = self.full.at[pl.ds(0, GROUP), 0, 0]
        elif name == "g":
            ref = self.full.at[pl.ds(0, GROUP), 0, 0, pl.ds(0, side * side // 2)]
        else:
            ref = self.full.at[pl.ds(0, GROUP), 0]
        return pltpu.make_async_copy(ref, ref, send if which == 0 else recv.at[lax.rem(q, DEPTH)])

    def gather_step(self, tick, i, before, after):
        t, there = self.tile(tick - FINISH - 1 - i)
        q = lax.div(t, GROUP)

        @pl.when(there & (t < self.gathered) & (lax.rem(t, GROUP) == GROUP - 1))
        def _():
            if before:
                self.gather_all(before, q, 1).wait()
                self.gather_all(before, q, 0).wait()
            if after == "f":
                for copy in self.keep(q):
                    copy.wait()
            if after:
                for copy in self.gather(after, q):
                    copy.start()
            if after == "d":
                for copy in self.keep(q):
                    copy.start()

    def part(self, tick, o):
        slot = lax.rem(tick + 1, DEPTH)
        self.in_parts(tick - 1, functools.partial(self.ring_wait, tick - 1, o))

        def at(back, what):
            t, there = self.tile(tick - back)
            pl.when(there)(lambda: what(t))

        def first(t):
            if o == 0:
                self.d2d(t).wait_recv()
                self.d2d(t).wait_send()
            self.sum_a(t, o)

        at(FINISH, lambda t: self.finish(t, slot, o))
        at(2, lambda t: self.sum_b(t, slot, o))
        at(1, first)
        at(3, lambda t: self.sum_a2(t, slot, o))
        at(4, lambda t: self.sum_b2(t, slot, o))

        def ring_start(one, two):
            for copy in self.ring(tick, o, one, two):
                copy.start()

        self.in_parts(tick, ring_start)

    def cross(self, tick):
        t, there = self.tile(tick)
        pl.when(there)(lambda: self.d2d(t).start())

    def others(self, tick):
        stages = ("d", "e", "f", "g", "h", "")
        for i in reversed(range(6)):
            self.gather_step(tick, i, stages[i - 1] if i else "", stages[i])

    def tick(self, tick):
        self.cross(tick)
        self.part(tick, 0)
        self.part(tick, 1)
        self.others(tick)


class Total:
    def __init__(self, place, sums, send, recv):
        self.place, self.sums, self.send, self.recv = place, sums, send, recv

    def over(self, k, value):
        members, me = self.place.members[k], self.place.positions[k]
        self.sums[k, me] = value
        here = self.sums.at[k, me]
        copies = [remote(here, here, self.send.at[k, i], self.recv.at[k, i], peer) for i, peer in enumerate(members) if i]
        for copy in copies:
            copy.start()
        for copy in copies:
            copy.wait()
        value = self.sums[k, 0]
        for i in range(1, len(members)):
            value = value + self.sums[k, i]
        return value


def gates(g, u, dact):
    s = jax.nn.sigmoid(g)
    silu = g * s
    act = (silu * u).astype(BF16)
    dup = (dact * silu).astype(BF16)
    dgate = (dact * u * (s + silu * (1.0 - s))).astype(BF16)
    return act, dgate, dup


def layers_kernel(x_hbm, dy_hbm, wg_hbm, wu_hbm, wd_hbm, full_ref, rest_ref, factor_ref, gate_hbm, up_hbm,
                  wg_ref, wu_ref, wd_ref, dy_ref, h_ref, a_ref, a0_ref, acc_ref, g_ref, u_ref, dact_ref, act_ref, dgu_ref,
                  own, mate, out, inn, out2, inn2, total, shard_ref, sq_ref, sums,
                  w_sem, x_sem, dy_sem, gu_sem, vs, vr, keep_sem, *pairs, mc, side, tiles, gathered, count):
    tokens, d = h_ref.shape
    tn = wg_ref.shape[2]
    chunks, blocks = tokens // mc, x_sem.shape[0]
    block = tokens // blocks
    place = Place(side)
    piece = d // (2 * side * side)
    sems = {name: pairs[2 * i:2 * i + 2] for i, name in enumerate(("d2d", "ring", "d", "e", "f", "g", "h"))}
    sems["keep"] = keep_sem
    exchange = Exchange(2 * tiles, gathered, place, (own, mate, out, inn, out2, inn2, total), sems, shard_ref, full_ref, rest_ref, sq_ref)

    def load_x(i):
        rows = ds(i, block)
        return pltpu.make_async_copy(x_hbm.at[rows], h_ref.at[rows], x_sem.at[i])

    def load_dy():
        return pltpu.make_async_copy(dy_hbm, dy_ref, dy_sem)

    def load_in(layer, t):
        slot = lax.rem(t, 2)
        return [
            pltpu.make_async_copy(wg_hbm.at[layer, :, ds(t, tn)], wg_ref.at[slot], w_sem.at[slot, 0]),
            pltpu.make_async_copy(wu_hbm.at[layer, :, ds(t, tn)], wu_ref.at[slot], w_sem.at[slot, 1]),
        ]

    def load_down(layer, t):
        slot = lax.rem(t, 2)
        return [pltpu.make_async_copy(wd_hbm.at[layer, ds(t, tn)], wd_ref.at[slot], w_sem.at[slot, 2])]

    def put_gu(t):
        slot = lax.rem(t, 2)
        return [
            pltpu.make_async_copy(g_ref.at[slot], gate_hbm.at[t], gu_sem.at[slot, 0]),
            pltpu.make_async_copy(u_ref.at[slot], up_hbm.at[t], gu_sem.at[slot, 1]),
        ]

    def get_gu(t):
        slot = lax.rem(t + 1, 2)
        return [
            pltpu.make_async_copy(gate_hbm.at[t], g_ref.at[slot], gu_sem.at[slot, 0]),
            pltpu.make_async_copy(up_hbm.at[t], u_ref.at[slot], gu_sem.at[slot, 1]),
        ]

    def start(copies):
        for copy in copies:
            copy.start()

    def wait(copies):
        for copy in copies:
            copy.wait()

    def ahead(layer, t, what):
        for load in what:
            pl.when(t + 1 < tiles)(lambda load=load: start(load(layer, t + 1)))
            wait(load(layer, t))

    def gu(c, t, a, slot):
        rows = pl.ds(c * mc, mc)
        a = a[rows, :]
        g_ref[slot, rows, :] = dot(a, wg_ref[lax.rem(t, 2)])
        u_ref[slot, rows, :] = dot(a, wu_ref[lax.rem(t, 2)])

    def da(c, t, right):
        dact_ref[c % 2] = dot_t(right[pl.ds(c * mc, mc), :], wd_ref[lax.rem(t, 2)])

    def epi(c, slot):
        rows = pl.ds(c * mc, mc)
        dact = dact_ref[c % 2].astype(BF16).astype(F32)
        act, dgate, dup = gates(g_ref[slot, rows, :], u_ref[slot, rows, :], dact)
        act_ref[rows, :] = act
        dgu_ref[rows, :tn] = dgate
        dgu_ref[rows, tn:] = dup

    def terms(n, left, right):
        term = [jnp.where(place.core == c, lax.rem(n, OWN), OWN + lax.rem(n, 2)) for c in range(2)]
        lanes, half = d // (2 * side), d // 2
        down = t_dot(act_ref[...], right[...]).astype(BF16)
        for o in range(2):
            for c in range(2):
                for i in range(side):
                    for j in range(side):
                        k = (i * side + j) * piece
                        own[term[c], o, k:k + piece, tn:] = down[
                            (o * side + i) * piece:(o * side + i + 1) * piece, (c * side + j) * lanes:(c * side + j + 1) * lanes
                        ]
        for c in range(2):
            at = left[:, c * half:(c + 1) * half]
            own[term[c], 0, :, :tn] = t_dot(at, dgu_ref[:, :tn]).astype(BF16)
            own[term[c], 1, :, :tn] = t_dot(at, dgu_ref[:, tn:]).astype(BF16)

    for i in range(blocks):
        load_x(i).start()
    start(load_in(0, 0) + load_down(0, 0))
    load_dy().start()
    greet([*place.members[0][1:], *place.members[1][1:]])
    sq_ref[...] = jnp.zeros_like(sq_ref)

    @pl.loop(0, blocks)
    def _(i):
        rows = ds(i, block)
        load_x(i).wait()
        a0_ref[rows, :] = norm_rows(h_ref[rows, :])
        acc_ref[rows, :] = jnp.zeros((block, d), F32)

    @pl.loop(0, tiles)
    def _(t):
        slot = lax.rem(t, 2)
        pl.when(t >= 2)(lambda: wait(put_gu(t - 2)))
        ahead(0, t, (load_in, load_down))

        def silu(c):
            rows = pl.ds(c * mc, mc)
            g, u = g_ref[slot, rows, :], u_ref[slot, rows, :]
            act_ref[rows, :] = (g * jax.nn.sigmoid(g) * u).astype(BF16)

        def down(c):
            rows = pl.ds(c * mc, mc)
            acc_ref[rows, :] += dot(act_ref[rows, :], wd_ref[slot])

        gu(0, t, a0_ref, slot)
        for c in range(chunks):
            if c + 1 < chunks:
                gu(c + 1, t, a0_ref, slot)
            silu(c)
            if c > 0:
                down(c - 1)
        down(chunks - 1)
        start(put_gu(t))

    start(load_in(1, 0) + load_down(1, 0))

    @pl.loop(0, blocks)
    def _(i):
        rows = ds(i, block)
        y = acc_ref[rows, :].astype(BF16).astype(F32)
        h = (h_ref[rows, :].astype(F32) + y).astype(BF16)
        h_ref[rows, :] = h
        a_ref[rows, :] = norm_rows(h)
        acc_ref[rows, :] = jnp.zeros((block, d), F32)

    wait(put_gu(tiles - 2) + put_gu(tiles - 1) + [load_dy()])
    start(get_gu(0))

    @pl.loop(0, tiles)
    def _(n):
        ahead(1, n, (load_in, load_down))

        def back(c):
            rows = pl.ds(c * mc, mc)
            slot = lax.rem(n, 2)
            acc_ref[rows, :] += dot_t(dgu_ref[rows, :tn], wg_ref[slot]) + dot_t(dgu_ref[rows, tn:], wu_ref[slot])

        gu(0, n, a_ref, 0)
        da(0, n, dy_ref)
        for c in range(1, chunks):
            gu(c, n, a_ref, 0)
            da(c, n, dy_ref)
            epi(c - 1, 0)
        back(0)
        epi(chunks - 1, 0)
        for c in range(1, chunks):
            back(c)
        exchange.tick(2 * n)
        terms(n, a_ref, dy_ref)
        exchange.tick(2 * n + 1)

    start(load_down(0, 0))

    @pl.loop(0, blocks)
    def _(i):
        rows = ds(i, block)
        da = acc_ref[rows, :].astype(BF16).astype(F32)
        h = h_ref[rows, :].astype(F32)
        ms = jnp.mean(h * h, -1, keepdims=True) + 1e-6
        r = lax.rsqrt(ms)
        along = jnp.mean(da * h, -1, keepdims=True)
        dn = (r * (da - h * (along / ms))).astype(BF16).astype(F32)
        h_ref[rows, :] = (dy_ref[rows, :].astype(F32) + dn).astype(BF16)

    @pl.loop(0, tiles)
    def _(t):
        slot = lax.rem(t + 1, 2)
        ahead(0, t, (load_down,))
        pl.when(t + 1 < tiles)(lambda: start(get_gu(t + 1)))
        wait(get_gu(t))
        da(0, t, h_ref)
        for c in range(1, chunks):
            da(c, t, h_ref)
            epi(c - 1, slot)
        epi(chunks - 1, slot)
        exchange.part(2 * tiles + t, 0)
        terms(tiles + t, a0_ref, h_ref)
        exchange.cross(2 * tiles + t)
        exchange.part(2 * tiles + t, 1)
        exchange.others(2 * tiles + t)

    @pl.loop(0, FINISH)
    def _(i):
        exchange.tick(3 * tiles + i)

    squares = Total(place, sums, vs, vr)
    value = jnp.full(factor_ref.shape, jnp.sum(sq_ref[...]), F32)
    for k in range(2):
        value = squares.over(k, value)
    factor_ref[...] = jnp.minimum(1.0, 0.5 * lax.rsqrt(value / count + 1e-30))


def layers(x, dy, wg, wu, wd, tn, side, gathered, count):
    t, d = x.shape
    ff = wg.shape[2]
    tiles = ff // tn
    piece, wide = d // (2 * side * side), tn + d // (2 * side)
    chunk = side * piece
    rows = side * chunk
    mc = t // 4
    hbm = pl.BlockSpec(memory_space=pl.ANY)
    rest = (2 * tiles - gathered, 2, piece, wide)
    return pl.pallas_call(
        functools.partial(layers_kernel, mc=mc, side=side, tiles=tiles, gathered=gathered, count=count),
        in_specs=[hbm] * 5,
        out_specs=[hbm, pl.BlockSpec(memory_space=pltpu.VMEM), pl.BlockSpec(memory_space=pltpu.VMEM), hbm, hbm],
        out_shape=[
            jax.ShapeDtypeStruct((gathered, 2, 2, side * side, piece, wide), BF16),
            jax.ShapeDtypeStruct(rest, BF16),
            jax.ShapeDtypeStruct((8, 128), F32),
            jax.ShapeDtypeStruct((tiles, t, tn), F32),
            jax.ShapeDtypeStruct((tiles, t, tn), F32),
        ],
        scratch_shapes=[
            pltpu.VMEM((2, d, tn), BF16), pltpu.VMEM((2, d, tn), BF16), pltpu.VMEM((2, tn, d), BF16),
            *[pltpu.VMEM((t, d), BF16)] * 4, pltpu.VMEM((t, d), F32),
            pltpu.VMEM((2, t, tn), F32), pltpu.VMEM((2, t, tn), F32), pltpu.VMEM((2, mc, tn), F32),
            pltpu.VMEM((t, tn), BF16), pltpu.VMEM((t, 2 * tn), BF16),
            pltpu.VMEM((OWN + 2, 2, rows, wide), BF16),
            pltpu.VMEM((MATE, 2, rows, wide), BF16),
            pltpu.VMEM((2, 2, chunk * 3 // 2, wide), BF16),
            pltpu.VMEM((DEPTH, 2, 2, chunk * 3 // 2, wide), BF16),
            pltpu.VMEM((2, 2, piece * 3 // 2, wide), BF16),
            pltpu.VMEM((DEPTH, 2, 2, piece * 3 // 2, wide), BF16),
            pltpu.VMEM((DEPTH, 2, chunk, wide), F32),
            pltpu.VMEM((2 * tiles, 2, piece, wide), BF16),
            pltpu.VMEM((piece, wide), F32),
            pltpu.VMEM((2, 2 * side, 8, 128), F32),
            DMA((2, 3)), DMA((8,)), DMA, DMA((2, 2)), DMA((2, 2 * side)), DMA((2, 2 * side)), DMA((DEPTH, 2)),
            DMA((2,)), DMA((MATE,)), DMA((2, 2)), DMA((DEPTH, 2, 2)),
            *[sem for name in range(5) for sem in (DMA, DMA((DEPTH,)))],
        ],
        compiler_params=pltpu.CompilerParams(
            vmem_limit_bytes=VLIM, collective_id=0, has_side_effects=True
        ),
        cost_estimate=pl.CostEstimate(flops=30 * t * d * ff, bytes_accessed=24 * d * ff, transcendentals=3 * t * ff),
        name="layers",
    )(x, dy, wg, wu, wd)[:3]


def adam_kernel(factor_ref, grad_ref, *refs, side, own):
    weights, moments, squares, new_w, new_m, new_v = (refs[i:i + 3] for i in [*range(0, 9, 3), *range(len(refs) - 9, len(refs), 3)])
    piece, wide = grad_ref.shape[-2:]
    tn = new_w[0].shape[2]
    lanes = wide - tn
    f = factor_ref[0, 0]

    def grad(c, o, i, j):
        if own:
            return grad_ref.at[0, c, o, i * side + j]
        return grad_ref.at[((i * side + j) if o == 0 else (j * side + i)) * 2 + c, 0, o]

    def step(k, at, g):
        g = g.astype(F32) * f
        m = 0.9 * moments[k][at] + 0.1 * g
        v = 0.95 * squares[k][at] + 0.05 * (g * g)
        w = weights[k][at].astype(F32)
        new_w[k][at] = (w - 0.02 * (m * lax.rsqrt(v + 1e-8) + 0.1 * w)).astype(BF16)
        new_m[k][at] = m
        new_v[k][at] = v

    for c in range(2):
        @pl.loop(0, side)
        def _(i):
            for j in range(side):
                for o in range(2):
                    step(o, (0, ds((c * side + i) * side + j, piece), slice(None)), grad(c, o, i, j)[:, :tn])
            for o in range(2):
                for j in range(side):
                    at = (0, ds(o * side + i, piece), slice((c * side + j) * lanes, (c * side + j + 1) * lanes))
                    step(2, at, grad(c, o, i, j)[:, tn:])


def adam(factor, grad, ws, ms, vs, so_far, tn, side, first, count):
    _, d, ff = ws[0].shape
    tiles = ff // tn
    at = lambda t: (1 - (t + first) // tiles, (t + first) % tiles)
    up = pl.BlockSpec((1, d, tn), lambda t: (at(t)[0], 0, at(t)[1]))
    down = pl.BlockSpec((1, tn, d), lambda t: (*at(t), 0))
    blocks = [up, up, down]
    own = not so_far
    size = sum(w.size for w in ws) * count // (2 * tiles)
    if own:
        grad_block = pl.BlockSpec((1, *grad.shape[1:]), lambda t: (t, 0, 0, 0, 0, 0))
    else:
        grad_block = pl.BlockSpec((grad.shape[0], 1, *grad.shape[2:]), lambda t: (0, t, 0, 0, 0))
    out = pl.pallas_call(
        functools.partial(adam_kernel, side=side, own=own),
        grid=(count,),
        in_specs=[
            pl.BlockSpec(factor.shape, lambda t: (0, 0), **ONE),
            grad_block,
            *blocks * 3,
            *[pl.BlockSpec(memory_space=pl.ANY)] * len(so_far),
        ],
        out_specs=blocks * 3,
        out_shape=[jax.ShapeDtypeStruct(a.shape, a.dtype) for a in (*ws, *ms, *vs)],
        input_output_aliases={11 + i: i for i in range(len(so_far))},
        compiler_params=pltpu.CompilerParams(vmem_limit_bytes=VLIM, dimension_semantics=("arbitrary",)),
        cost_estimate=pl.CostEstimate(flops=20 * size, bytes_accessed=22 * size, transcendentals=size),
        name="adam_own" if own else "adam_rest",
    )(factor, grad, *ws, *ms, *vs, *so_far)
    return tuple(out)


def solution(mesh):
    side = math.isqrt(mesh.shape["dp"] // 2)

    def step(x, dy, *arrays):
        ws, ms, vs = (arrays[i:i + 3] for i in (0, 3, 6))
        x, dy = x[0], dy[0]
        tn = x.shape[1] // side
        tiles = ws[0].shape[0] * ws[0].shape[2] // tn
        gathered = tiles * 6 // 10
        full, rest, factor = layers(x, dy, *ws, tn, side, gathered, sum(w.size for w in ws))
        rest = lax.all_gather(rest, "dp")
        new = adam(factor, full, ws, ms, vs, (), tn, side, 0, gathered)
        return adam(factor, rest, ws, ms, vs, new, tn, side, gathered, tiles - gathered)

    return jax.shard_map(
        step,
        mesh=mesh,
        in_specs=(P(("rep", "dp"), None, None),) * 2 + (P(None, None, None),) * 9,
        out_specs=(P("rep", None, None),) * 9,
        check_vma=False,
    )
```
